256 devices in a mesh: mkt: 32 (over z, x_lo, core), draw: 4 (over y), nest: 2 (over x_hi).
Axes of the slice: x: 4 (x_hi: 2, x_lo: 2; x = x_hi * 2 + x_lo), y: 4, z: 8, core: 2. Of those that a mesh axis runs over, the one named last changes fastest.
Arguments:
- features: bfloat16 [32, 512, 1024], P(None, 'mkt'), may hold values from -1.5 to 1.5
- taste_draws: bfloat16 [1024, 32, 512], P('mkt', None, 'draw'), may hold values from -4 to 4
- taste_scale: float32 [32], replicated, may hold values from 0.2 to 1
- nest_param: float32 [16], P('nest'), may hold values from 0.3 to 0.95
- members: int32 [16, 48], P('nest'), may hold values from -1 to 511, as said below
- log_share: float32 [512, 1024], P('mkt'), may hold values from -10 to -7
Outputs:
- mean_utility: float32 [1024, 768], P('mkt', 'nest')
- model_share: float32 [1024, 768], P('mkt', 'nest')
The draws below stay inside these ranges and needn't reach their ends.
Inputs may be any that keep to these rules, and one draw needn't show every extreme that they name: `members`: every product id 0 to 511 stands in exactly one slot; in each nest's row the ids fill the first slots and -1 fills the rest; each nest holds at least 16 products, and some nest fills all 48 slots.
All inputs are finite; a program needn't handle non-finite values.
Results may differ from the reference program's by a relative error of at most 0.0013.
The reference program's roundings to bfloat16 on the way count: a program that leaves them out, or rounds other values in their place, can miss the bound.
Values may be sent and summed in bfloat16 or wider, within the bound.
No kernel may reach another device: no remote copies, remote signals or barrier semaphores. Data moves between devices by JAX's collectives and lax.ppermute only.
A program may use at most 64 MiB of HBM per device.

```python
import math
import jax
import jax.numpy as jnp
from jax import lax

K = 32
J = 512
G = 16
SLOTS = 48
MARKETS = 1024
DRAWS = 512
ITERS = 3


def draw_members(key, part):
    first_key, second_key, third_key = jax.random.split(key, 3)
    baseline_size = J // G
    half_size = baseline_size // 2
    shifts = jax.random.randint(first_key, (G // 2,), 0, half_size + 1).astype(jnp.int32)
    shifts = shifts.at[0].set(half_size)
    sizes = jnp.stack([baseline_size + shifts, baseline_size - shifts], axis=1).reshape(G)
    nest_order = jax.random.permutation(second_key, G)
    sizes = sizes[nest_order].astype(jnp.int32)
    offsets = (jnp.cumsum(sizes) - sizes).astype(jnp.int32)
    products = jax.random.permutation(third_key, J).astype(jnp.int32)
    slot_index = jnp.arange(SLOTS, dtype=jnp.int32)[None, :]
    position = jnp.minimum(offsets[:, None] + slot_index, J - 1)
    return jnp.where(slot_index < sizes[:, None], products[position], -1).astype(jnp.int32)


def steps_of(own_key, shape, cuts, least, top_value):
    loudness, own = 1.0, jax.random.fold_in(own_key, 6)
    for dim, blocks in cuts:
        draws = jnp.exp(jax.random.uniform(jax.random.fold_in(own, dim), (blocks,), jnp.float32, least / len(cuts), top_value / len(cuts)))
        loudness = loudness * jnp.repeat(draws, shape[dim] // blocks).reshape([-1 if axis == dim else 1 for axis in range(len(shape))])
    return loudness


def noise(stream_key, extent, deviation, bound, shards=(), kind=jnp.bfloat16):
    loudness = steps_of(stream_key, extent, shards, -0.22, 0.18) if shards else 1.0
    values = jax.random.normal(stream_key, extent, jnp.float32) * deviation * loudness
    return jnp.minimum(jnp.maximum(values, -bound), bound).astype(kind)


def setup_inputs(seed: int = 0) -> dict:
    seeds = jax.random.split(jax.random.key(seed), 7)
    return {
        "features": noise(seeds[0], (K, J, MARKETS), 0.25, 1.5, ((1, 32),)),
        "taste_draws": noise(seeds[1], (MARKETS, K, DRAWS), 1.0, 4.0, ((0, 32), (2, 4))),
        "taste_scale": jnp.clip(jax.random.uniform(seeds[2], (K,), jnp.float32, 0.2, 1.0), 0.2, 1.0),
        "nest_param": jnp.clip(jnp.exp(math.log(0.95) - 1.1526795 * jax.random.uniform(seeds[3], (G,), jnp.float32) ** steps_of(seeds[3], (G,), ((0, 2),), -0.2, 0.2)), 0.3, 0.95),
        "members": draw_members(jax.random.fold_in(seeds[6], 71), 0),
        "log_share": jnp.clip(-10.0 + 3.0 * jax.random.uniform(seeds[5], (J, MARKETS), jnp.float32) ** steps_of(seeds[5], (J, MARKETS), ((0, 32),), -0.2, 0.2), -10.0, -7.0),
    }


def revise(value_slot, slot_share, target, nest_rate, occupied):
    safe_share = jnp.where(occupied[None, :], slot_share, 1.0)
    moved_value = value_slot + (1.0 - nest_rate)[None, :] * (target - jnp.log(safe_share))
    return jnp.where(occupied[None, :], moved_value, 0.0)


def reference(features, taste_draws, taste_scale, nest_param, members, log_share):
    columns = G * SLOTS
    product_ids = members.reshape(columns).astype(jnp.int32)
    occupied = product_ids >= 0
    safe_ids = jnp.maximum(product_ids, 0).astype(jnp.int32)
    live_flag = occupied.astype(jnp.float32)
    picked = jnp.take(features, safe_ids, axis=1)
    slot_features = jnp.where(occupied[None, :, None], picked, jnp.zeros((), jnp.bfloat16))
    slot_features = jnp.transpose(slot_features, (2, 0, 1))
    slot_log = jnp.transpose(jnp.take(log_share, safe_ids, axis=0), (1, 0))
    outside = 1.0 - jnp.sum(jnp.exp(log_share), axis=0)
    start_value = jnp.where(occupied[None, :], slot_log - jnp.log(outside)[:, None], 0.0)
    taste_matrix = (taste_scale[None, :, None] * taste_draws.astype(jnp.float32)).astype(jnp.bfloat16)
    nest_rate = jnp.repeat(nest_param, SLOTS)
    block_size = math.gcd(MARKETS, 8)
    block_count = MARKETS // block_size

    def market_block(operands):
        char_block, taste_block, value_block, target_block = operands
        mean_utility_part = jnp.einsum("bks,bkr->bsr", char_block.astype(jnp.float32), taste_block.astype(jnp.float32), precision=lax.Precision.HIGHEST)
        share_block = jnp.zeros_like(value_block)
        for iteration in range(ITERS):
            utility = live_flag[None, :, None] * jnp.exp((value_block[:, :, None] + mean_utility_part) / nest_rate[None, :, None])
            grouped = utility.reshape(block_size, G, SLOTS, DRAWS)
            inner_sum = jnp.sum(grouped, axis=2)
            inclusive_value = jnp.exp(nest_param[None, :, None] * jnp.log(inner_sum))
            nest_ratio = inclusive_value / (inner_sum * (1.0 + jnp.sum(inclusive_value, axis=1))[:, None, :])
            share_block = jnp.sum(grouped * nest_ratio[:, :, None, :], axis=3).reshape(block_size, columns) / DRAWS
            value_block = revise(value_block, share_block, target_block, nest_rate, occupied)
        return value_block, share_block

    operands = (slot_features.reshape(block_count, block_size, K, columns), taste_matrix.reshape(block_count, block_size, K, DRAWS), start_value.reshape(block_count, block_size, columns), slot_log.reshape(block_count, block_size, columns))
    value_out, share_out = lax.map(market_block, operands)
    return value_out.reshape(MARKETS, columns), share_out.reshape(MARKETS, columns)
```

```python
import functools
import math

import jax
import jax.numpy as jnp
from jax import lax
from jax.experimental import pallas as pl
from jax.experimental.pallas import tpu as pltpu
from jax.sharding import PartitionSpec as P

ITERS = 3
BLOCKS = 32
QUAD = 4
K = 32
PROD = 16
SLOTS = 48
NESTS = 16
HALF = 8
DRAWS = 512
MARKETS = 1024
LANES = 128
ROWS = 24
LOG2E = 1.0 / math.log(2.0)
LOW = -1e30
TINY = 1.1754944e-38
f32, bf16, i32 = jnp.float32, jnp.bfloat16, jnp.int32
VMEM = pl.BlockSpec(memory_space=pltpu.VMEM)
SMEM = pl.BlockSpec(memory_space=pltpu.SMEM)


def iota(shape, dim):
    return lax.broadcasted_iota(i32, shape, dim)


def dot(a, b):
    return lax.dot_general(a, b, (((1,), (0,)), ((), ())), preferred_element_type=f32)


def dot_t(a, b):
    return lax.dot_general(a, b, (((1,), (1,)), ((), ())), preferred_element_type=f32)


def pack(me_ref, f_ref, l_ref, out_ref, g_ref, o_ref, s_ref):
    base = me_ref[0] * QUAD
    market = iota((MARKETS, LANES), 0)
    lane = iota((MARKETS, LANES), 1)
    pick = jnp.where(market == (lane % BLOCKS) * 32 + base + lane // BLOCKS, 1.0, 0.0).astype(bf16)
    g_ref[...] = dot(f_ref[...].reshape(K * PROD, MARKETS), pick)
    log = l_ref[...]
    high = log.astype(bf16)
    rest = log - high.astype(f32)
    middle = rest.astype(bf16)
    low = (rest - middle.astype(f32)).astype(bf16)
    logs = dot(jnp.concatenate([high, middle, low], axis=0), pick)
    spread = jnp.where(iota((BLOCKS, LANES), 0) == iota((BLOCKS, LANES), 1) % BLOCKS, 1.0, 0.0).astype(bf16)
    own = iota((LANES, LANES), 0) // K == iota((LANES, LANES), 1) // BLOCKS
    for j in range(PROD):
        part = g_ref[pl.ds(j, K, stride=PROD), :]
        part = jnp.where(own, jnp.concatenate([part] * QUAD, axis=0), 0.0).astype(bf16)
        o_ref[pl.ds(j, BLOCKS, stride=PROD), :] = dot_t(spread, part)
    out_ref[:, :PROD, :] = o_ref[...].reshape(BLOCKS, PROD, LANES).astype(bf16)
    own = (iota((LANES, LANES), 0) // PROD) % QUAD == iota((LANES, LANES), 1) // BLOCKS
    first = jnp.concatenate([logs[:PROD]] * QUAD + [logs[PROD : 2 * PROD]] * QUAD, axis=0)
    second = jnp.concatenate([logs[2 * PROD :]] * QUAD + [jnp.zeros((64, LANES), f32)], axis=0)
    s_ref[...] = jnp.zeros_like(s_ref)
    s_ref[pl.ds(0, BLOCKS, stride=8), :] = dot_t(spread, jnp.where(own, first, 0.0).astype(bf16))
    s_ref[pl.ds(1, BLOCKS, stride=8), :] = dot_t(spread, jnp.where(own, second, 0.0).astype(bf16))
    out_ref[:, PROD:, :] = s_ref[...].reshape(BLOCKS, 8, LANES).astype(bf16)


def across(x):
    return jnp.concatenate([x] * (DRAWS // LANES), axis=1)


def contract(me_ref, x_ref, t0_ref, t1_ref, t2_ref, t3_ref, scale_ref, near_ref, far_ref, out_ref,
             hot_ref, slot_ref, taste_ref, mu_ref, e_ref, v_ref, t_ref, s_ref, l_ref, y_ref):
    near, far = near_ref[...], far_ref[...]
    first = me_ref[1] == 0
    table = jnp.concatenate([jnp.where(first, near, far), jnp.where(first, far, near)], axis=0)
    rate = jnp.broadcast_to(table[:, SLOTS : SLOTS + 1], (NESTS, LANES))
    to_two = LOG2E / rate
    gain = (1.0 - rate) * to_two
    ids = table.astype(i32)
    wide = iota((NESTS, DRAWS), 1)
    narrow = iota((NESTS, LANES), 1)

    for t in range(SLOTS):
        here = jnp.broadcast_to(ids[:, t : t + 1], (NESTS, LANES))
        hot_ref[t * NESTS : (t + 1) * NESTS, :] = jnp.where(across(here) == wide, 1.0, 0.0).astype(bf16)
    x = x_ref[:, :PROD, :].reshape(BLOCKS * PROD, LANES)
    slot_ref[...] = dot(hot_ref[...], x).astype(bf16)

    l_ref[...] = x_ref[:, PROD:, :].astype(f32).reshape(BLOCKS * 8, LANES)
    top = l_ref[pl.ds(0, BLOCKS, stride=8), :]
    rest = l_ref[pl.ds(1, BLOCKS, stride=8), :]
    both = jnp.concatenate([top, rest], axis=1).astype(bf16)
    for t in range(SLOTS):
        here = jnp.broadcast_to(ids[:, t : t + 1], (NESTS, LANES))
        y_ref[t * NESTS : (t + 1) * NESTS, :] = jnp.where((here >> 4) == narrow, 1.0, 0.0).astype(bf16)
    rows = dot(y_ref[:, :BLOCKS], both)
    lane2 = iota((NESTS, 2 * LANES), 1) % PROD
    for t in range(SLOTS):
        here = jnp.broadcast_to(ids[:, t : t + 1], (NESTS, LANES)) & 15
        here = jnp.concatenate([here, here], axis=1)
        cut = rows[t * NESTS : (t + 1) * NESTS, :]
        slot = jnp.where(here == lane2, cut, 0.0).astype(bf16)
        hot_ref[t * NESTS : (t + 1) * NESTS, : 2 * LANES] = slot
    copies = jnp.where(
        (iota((2 * LANES, DRAWS), 0) // PROD) % QUAD == iota((2 * LANES, DRAWS), 1) // LANES, 1.0, 0.0
    ).astype(bf16)
    target = dot(hot_ref[:, : 2 * LANES], copies)
    whole = (top + pltpu.roll(top, 64, 1)) + rest
    shares = jnp.exp(whole)
    column = iota((BLOCKS, LANES), 1)
    for q in range(QUAD):
        inside = jnp.where(column // PROD == q, shares, 0.0)
        outside = 1.0 - jnp.sum(jnp.sum(inside, axis=1, keepdims=True), axis=0, keepdims=True)
        outside = jnp.broadcast_to(jnp.log(outside), (NESTS, LANES))
        for t in range(SLOTS):
            here = jnp.broadcast_to(ids[:, t : t + 1], (NESTS, LANES))
            goal = target[t * NESTS : (t + 1) * NESTS, q * LANES : (q + 1) * LANES]
            t_ref[q, t] = goal + math.log(DRAWS)
            v_ref[q, t] = jnp.where(here >= 0, (goal - outside) * to_two, LOW)

    square = iota((K, K), 0) == iota((K, K), 1)
    scale = jnp.sum(jnp.where(square, jnp.broadcast_to(scale_ref[...], (K, K)), 0.0), axis=1, keepdims=True)
    scale = jnp.broadcast_to(scale, (K, LANES))
    taste_ref[...] = jnp.zeros_like(taste_ref)
    for q in range(QUAD):
        for b, ref in enumerate((t0_ref, t1_ref, t2_ref, t3_ref)):
            taste = (scale * ref[q].astype(f32)).astype(bf16)
            taste_ref[q, q * K : (q + 1) * K, b * LANES : (b + 1) * LANES] = taste
    for q in range(QUAD):
        mu = dot(slot_ref[...], taste_ref[q])
        mu_ref[q] = mu.reshape(SLOTS, NESTS, DRAWS) * across(to_two)[None]

    less = across(rate - 1.0)

    def step(_, carry):
        for q in range(QUAD):
            inner = jnp.zeros((NESTS, DRAWS), f32)
            for t in range(SLOTS):
                e = jnp.exp2(mu_ref[q, t] + across(v_ref[q, t]))
                e_ref[q, t] = e
                inner = inner + e
            power = jnp.exp2(less * (jnp.log(inner) * LOG2E))
            total = 1.0 + jnp.sum(power * inner, axis=0, keepdims=True)
            weight = power / total
            for t in range(SLOTS):
                p = e_ref[q, t] * weight
                p = (p[:, :128] + p[:, 128:256]) + (p[:, 256:384] + p[:, 384:])
                share = jnp.broadcast_to(jnp.sum(p, axis=1, keepdims=True), (NESTS, LANES))
                s_ref[q, t] = share
                v_ref[q, t] = v_ref[q, t] + gain * (t_ref[q, t] - jnp.log(jnp.maximum(share, TINY)))
        return carry

    lax.fori_loop(0, ITERS, step, 0)
    back = rate * math.log(2.0)
    for q in range(QUAD):
        values = jnp.zeros((NESTS, LANES), f32)
        shares = jnp.zeros((NESTS, LANES), f32)
        for t in range(SLOTS):
            values = jnp.where(narrow == t, v_ref[q, t], values)
            shares = jnp.where(narrow == t + 64, s_ref[q, t], shares)
        values = jnp.where(ids >= 0, values * back, 0.0)
        both = jnp.where(narrow < SLOTS, values, shares * (1.0 / DRAWS))
        for d in range(4):
            for n in range(2):
                out_ref[2 * d + n, q * HALF : (q + 1) * HALF, :] = both[n * HALF : (n + 1) * HALF]


def unpack(r_ref, value_ref, share_ref):
    for g in range(HALF):
        part = r_ref[pl.ds(g, 32, stride=HALF), :]
        value_ref[:, g * SLOTS : (g + 1) * SLOTS] = part[:, :SLOTS]
        share_ref[:, g * SLOTS : (g + 1) * SLOTS] = part[:, 64 : 64 + SLOTS]


def shards(features, taste_draws, taste_scale, nest_param, members, log_share):
    d, n = lax.axis_index("draw"), lax.axis_index("nest")
    me = jnp.stack([d * 2 + n, n]).astype(i32)
    send = pl.pallas_call(
        pack,
        name="pack",
        out_shape=jax.ShapeDtypeStruct((BLOCKS, ROWS, LANES), bf16),
        in_specs=[SMEM, VMEM, VMEM],
        out_specs=VMEM,
        scratch_shapes=[
            pltpu.VMEM((K * PROD, LANES), f32),
            pltpu.VMEM((BLOCKS * PROD, LANES), f32),
            pltpu.VMEM((BLOCKS * 8, LANES), f32),
        ],
    )(me, features, log_share)
    recv = lax.all_to_all(send, "mkt", split_axis=0, concat_axis=0, tiled=True)

    near = jnp.concatenate(
        [members.astype(f32), nest_param[:, None], jnp.zeros((HALF, LANES - SLOTS - 1), f32)], axis=1
    )
    far = lax.ppermute(near, "nest", [(0, 1), (1, 0)])
    tastes = []
    for shift in range(4):
        to = (d + shift) % 4
        piece = lax.dynamic_slice_in_dim(taste_draws, to * 8 + n * QUAD, QUAD, 0)
        if shift:
            piece = lax.ppermute(piece, "draw", [(i, (i + shift) % 4) for i in range(4)])
        tastes.append(piece)

    big = (QUAD, SLOTS, NESTS, DRAWS)
    small = (QUAD, SLOTS, NESTS, LANES)
    results = pl.pallas_call(
        contract,
        name="contract",
        out_shape=jax.ShapeDtypeStruct((8, 32, LANES), f32),
        in_specs=[SMEM] + [VMEM] * 8,
        out_specs=VMEM,
        scratch_shapes=[
            pltpu.VMEM((SLOTS * NESTS, DRAWS), bf16),
            pltpu.VMEM((SLOTS * NESTS, LANES), bf16),
            pltpu.VMEM((QUAD, QUAD * K, DRAWS), bf16),
            pltpu.VMEM(big, f32),
            pltpu.VMEM(big, f32),
            pltpu.VMEM(small, f32),
            pltpu.VMEM(small, f32),
            pltpu.VMEM(small, f32),
            pltpu.VMEM((BLOCKS * 8, LANES), f32),
            pltpu.VMEM((SLOTS * NESTS, LANES), bf16),
        ],
        compiler_params=pltpu.CompilerParams(vmem_limit_bytes=48 * 1024 * 1024),
    )(me, recv, *tastes, taste_scale.reshape(1, K), near, far)
    gathered = lax.all_to_all(results, ("draw", "nest"), split_axis=0, concat_axis=0, tiled=True)
    shape = jax.ShapeDtypeStruct((32, HALF * SLOTS), f32)
    return pl.pallas_call(
        unpack, name="unpack", out_shape=(shape, shape), in_specs=[VMEM], out_specs=(VMEM, VMEM)
    )(gathered.reshape(256, LANES))


def solution(mesh):
    in_specs = (
        P(None, "mkt", None),
        P("mkt", None, "draw"),
        P(),
        P("nest"),
        P("nest", None),
        P("mkt", None),
    )
    out_specs = (P("mkt", "nest"), P("mkt", "nest"))
    return jax.shard_map(shards, mesh=mesh, in_specs=in_specs, out_specs=out_specs, check_vma=False)
```

```python
import functools
import math

import jax
import jax.numpy as jnp
from jax import lax
from jax.experimental import pallas as pl
from jax.experimental.pallas import tpu as pltpu
from jax.sharding import PartitionSpec as P

ITERS = 3
BLOCKS = 32
QUAD = 4
K = 32
PROD = 16
SLOTS = 48
NESTS = 16
HALF = 8
DRAWS = 512
MARKETS = 1024
LANES = 128
ROWS = 24
LOG2E = 1.0 / math.log(2.0)
LOW = -1e30
TINY = 1.1754944e-38
EMPTY = 32 * 16 + 15
PLACES = [(o, t) for o in range(2) for t in range(SLOTS)]
f32, bf16, i32 = jnp.float32, jnp.bfloat16, jnp.int32
VMEM = pl.BlockSpec(memory_space=pltpu.VMEM)


def iota(shape, dim):
    return lax.broadcasted_iota(i32, shape, dim)


def dot(a, b):
    return lax.dot_general(a, b, (((1,), (0,)), ((), ())), preferred_element_type=f32)


def dot_t(a, b):
    return lax.dot_general(a, b, (((1,), (1,)), ((), ())), preferred_element_type=f32)


def pack(f_ref, l_ref, out_ref, g_ref, o_ref, s_ref):
    base = (lax.axis_index("draw") * 2 + lax.axis_index("nest")) * QUAD
    market = iota((MARKETS, LANES), 0)
    lane = iota((MARKETS, LANES), 1)
    pick = jnp.where(market == (lane % BLOCKS) * 32 + base + lane // BLOCKS, 1.0, 0.0).astype(bf16)
    g_ref[...] = dot(f_ref[...].reshape(K * PROD, MARKETS), pick)
    log = l_ref[...]
    high = log.astype(bf16)
    rest = log - high.astype(f32)
    middle = rest.astype(bf16)
    low = (rest - middle.astype(f32)).astype(bf16)
    logs = dot(jnp.concatenate([high, middle, low], axis=0), pick)
    spread = jnp.where(iota((BLOCKS, LANES), 0) == iota((BLOCKS, LANES), 1) % BLOCKS, 1.0, 0.0).astype(bf16)
    own = iota((LANES, LANES), 0) // K == iota((LANES, LANES), 1) // BLOCKS
    for j in range(PROD):
        part = g_ref[pl.ds(j, K, stride=PROD), :]
        part = jnp.where(own, jnp.concatenate([part] * QUAD, axis=0), 0.0).astype(bf16)
        o_ref[pl.ds(j, BLOCKS, stride=PROD), :] = dot_t(spread, part)
    out_ref[:, :PROD, :] = o_ref[...].reshape(BLOCKS, PROD, LANES).astype(bf16)
    own = (iota((LANES, LANES), 0) // PROD) % QUAD == iota((LANES, LANES), 1) // BLOCKS
    first = jnp.concatenate([logs[:PROD]] * QUAD + [logs[PROD : 2 * PROD]] * QUAD, axis=0)
    second = jnp.concatenate([logs[2 * PROD :]] * QUAD + [jnp.zeros((64, LANES), f32)], axis=0)
    s_ref[...] = jnp.zeros_like(s_ref)
    s_ref[pl.ds(0, BLOCKS, stride=8), :] = dot_t(spread, jnp.where(own, first, 0.0).astype(bf16))
    s_ref[pl.ds(1, BLOCKS, stride=8), :] = dot_t(spread, jnp.where(own, second, 0.0).astype(bf16))
    out_ref[:, PROD:, :] = s_ref[...].reshape(BLOCKS, 8, LANES).astype(bf16)


def across(x):
    return jnp.concatenate([x] * (DRAWS // LANES), axis=1)


def arrange(near_ref, far_ref, scale_ref, table_ref, hot_ref, pick_ref, mask_ref):
    near, far = near_ref[...], far_ref[...]
    first = lax.axis_index("nest") == 0
    table = jnp.concatenate([jnp.where(first, near, far), jnp.where(first, far, near)], axis=0)
    table_ref[:NESTS, :] = table
    square = iota((K, K), 0) == iota((K, K), 1)
    scale = jnp.sum(jnp.where(square, jnp.broadcast_to(scale_ref[...], (K, K)), 0.0), axis=1, keepdims=True)
    table_ref[NESTS:, :] = jnp.broadcast_to(scale, (K, LANES))
    ids = table.astype(i32)
    ids = jnp.where(ids < 0, EMPTY, ids)
    wide, narrow = iota((HALF, DRAWS), 1), iota((HALF, LANES), 1)
    for b in range(0, len(PLACES), 2):
        hot, pick, mask = [], [], []
        for o, t in PLACES[b : b + 2]:
            here = jnp.broadcast_to(ids[o * HALF : (o + 1) * HALF, t : t + 1], (HALF, LANES))
            hot.append(jnp.where(across(here) == wide, 1.0, 0.0))
            pick.append(jnp.where((here >> 4) == narrow, 1.0, 0.0))
            mask.append(jnp.where((here & 15) == (narrow & 15), 1.0, 0.0))
        rows = slice(b * HALF, (b + 2) * HALF)
        hot_ref[rows, :] = jnp.concatenate(hot, axis=0).astype(bf16)
        pick_ref[rows, :] = jnp.concatenate(pick, axis=0).astype(bf16)
        mask_ref[rows, :] = jnp.concatenate(mask, axis=0).astype(bf16)


def contract(x_ref, t0_ref, t1_ref, t2_ref, t3_ref, table_ref, hot_ref, pick_ref, mask_ref, out_ref,
             slot_ref, taste_ref, mu_ref, e_ref, v_ref, t_ref, l_ref):
    table = [table_ref[o * HALF : (o + 1) * HALF, :] for o in range(2)]
    rate = [jnp.broadcast_to(x[:, SLOTS : SLOTS + 1], (HALF, LANES)) for x in table]
    inverse = [1.0 / x for x in rate]
    to_two = [across(LOG2E * x) for x in inverse]
    gain = [(1.0 - x) * y for x, y in zip(rate, inverse)]
    less = [across(x - 1.0) for x in rate]
    narrow = iota((HALF, LANES), 1)

    l_ref[...] = x_ref[:, PROD:, :].astype(f32).reshape(BLOCKS * 8, LANES)
    top = l_ref[pl.ds(0, BLOCKS, stride=8), :]
    rest = l_ref[pl.ds(1, BLOCKS, stride=8), :]
    both = jnp.concatenate([top, rest], axis=1)
    lane = iota((BLOCKS, 2 * LANES), 1)
    lows = (iota((BLOCKS, 2 * LANES), 0) == 0) & (lane < 64) & (lane % PROD == PROD - 1)
    both = jnp.concatenate([both, jnp.where(lows, LOW, 0.0), jnp.zeros((64, 2 * LANES), f32)], axis=0).astype(bf16)
    rows = dot(pick_ref[...], both).astype(bf16)
    mask = mask_ref[...]
    rows = rows * jnp.concatenate([mask, mask], axis=1)
    copies = jnp.where(
        (iota((2 * LANES, DRAWS), 0) // PROD) % QUAD == iota((2 * LANES, DRAWS), 1) // LANES, 1.0, 0.0
    ).astype(bf16)
    target = dot(rows, copies)
    whole = (top + pltpu.roll(top, 64, 1)) + rest
    shares = jnp.exp(whole)
    column = iota((BLOCKS, LANES), 1)
    outside = []
    for q in range(QUAD):
        inside = jnp.where(column // PROD == q, shares, 0.0)
        total = 1.0 - jnp.sum(jnp.sum(inside, axis=1, keepdims=True), axis=0, keepdims=True)
        outside.append(lax.log2(jnp.broadcast_to(total, (HALF, LANES))))

    x = x_ref[:, :PROD, :].reshape(BLOCKS * PROD, LANES)
    slot_ref[...] = dot(hot_ref[...], x).astype(bf16)
    scale = table_ref[NESTS:, :]
    taste_ref[...] = jnp.zeros_like(taste_ref)
    for q in range(QUAD):
        for b, ref in enumerate((t0_ref, t1_ref, t2_ref, t3_ref)):
            taste = (scale * ref[q].astype(f32)).astype(bf16)
            taste_ref[q, q * K : (q + 1) * K, b * LANES : (b + 1) * LANES] = taste

    def weights(inner):
        power = [jnp.exp2(x * lax.log2(y)) for x, y in zip(less, inner)]
        total = jnp.sum(power[0] * inner[0] + power[1] * inner[1], axis=0, keepdims=True)
        total = (1.0 + total) * DRAWS
        return [x / total for x in power]

    def first_half(q, b, inner, value, mu):
        o = PLACES[b][0]
        e = jnp.exp2(mu + across(value))
        e_ref[q, b] = e
        inner[o] = inner[o] + e

    def second_half(q, b, weight):
        o = PLACES[b][0]
        p = e_ref[q, b] * weight[o]
        p = (p[:, :128] + p[:, 128:256]) + (p[:, 256:384] + p[:, 384:])
        share = jnp.broadcast_to(jnp.sum(p, axis=1, keepdims=True), (HALF, LANES))
        value = v_ref[q, b] + gain[o] * (t_ref[q, b] - lax.log2(jnp.maximum(share, TINY)))
        return value, share

    zeros = jnp.zeros((HALF, DRAWS), f32)
    weight = [None] * QUAD
    count = len(PLACES)
    for q in range(QUAD):
        mu = dot(slot_ref[...], taste_ref[q])
        inner = [zeros, zeros]
        for b, (o, _) in enumerate(PLACES):
            part = mu[b * HALF : (b + 1) * HALF] * to_two[o]
            mu_ref[q, b] = part
            goal = target[b * HALF : (b + 1) * HALF, q * LANES : (q + 1) * LANES] * LOG2E
            t_ref[q, b] = goal
            value = (goal - outside[q]) * inverse[o]
            v_ref[q, b] = value
            first_half(q, b, inner, value, part)
        weight[q] = weights(inner)

    for _ in range(ITERS - 1):
        old = list(weight)
        for q in range(QUAD + 1):
            inner = [zeros, zeros]
            for b in range(count):
                if q < QUAD:
                    v_ref[q, b] = second_half(q, b, old[q])[0]
                if q:
                    first_half(q - 1, b, inner, v_ref[q - 1, b], mu_ref[q - 1, b])
            if q:
                weight[q - 1] = weights(inner)

    back = [x * math.log(2.0) for x in rate]
    for q in range(QUAD):
        values = [jnp.zeros((HALF, LANES), f32)] * 2
        shares = [jnp.zeros((HALF, LANES), f32)] * 2
        for b, (o, t) in enumerate(PLACES):
            value, share = second_half(q, b, weight[q])
            values[o] = jnp.where(narrow == t, value, values[o])
            shares[o] = jnp.where(narrow == t + 64, share, shares[o])
        for n in range(2):
            value = jnp.where(table[n] >= 0.0, values[n] * back[n], 0.0)
            both = jnp.where(narrow < SLOTS, value, shares[n])
            for d in range(4):
                out_ref[2 * d + n, q * HALF : (q + 1) * HALF, :] = both


def unpack(r_ref, value_ref, share_ref):
    for g in range(HALF):
        part = r_ref[pl.ds(g, 32, stride=HALF), :]
        value_ref[:, g * SLOTS : (g + 1) * SLOTS] = part[:, :SLOTS]
        share_ref[:, g * SLOTS : (g + 1) * SLOTS] = part[:, 64 : 64 + SLOTS]


def shards(features, taste_draws, taste_scale, nest_param, members, log_share):
    send = pl.pallas_call(
        pack,
        name="pack",
        out_shape=jax.ShapeDtypeStruct((BLOCKS, ROWS, LANES), bf16),
        in_specs=[VMEM, VMEM],
        out_specs=VMEM,
        scratch_shapes=[
            pltpu.VMEM((K * PROD, LANES), f32),
            pltpu.VMEM((BLOCKS * PROD, LANES), f32),
            pltpu.VMEM((BLOCKS * 8, LANES), f32),
        ],
    )(features, log_share)
    recv = lax.all_to_all(send, "mkt", split_axis=0, concat_axis=0, tiled=True)

    near = jnp.concatenate(
        [members.astype(f32), nest_param[:, None], jnp.zeros((HALF, LANES - SLOTS - 1), f32)], axis=1
    )
    far = lax.ppermute(near, "nest", [(0, 1), (1, 0)])
    rows = len(PLACES) * HALF
    plan = pl.pallas_call(
        arrange,
        name="arrange",
        out_shape=(
            jax.ShapeDtypeStruct((NESTS + K, LANES), f32),
            jax.ShapeDtypeStruct((rows, DRAWS), bf16),
            jax.ShapeDtypeStruct((rows, LANES), bf16),
            jax.ShapeDtypeStruct((rows, LANES), bf16),
        ),
        in_specs=[VMEM] * 3,
        out_specs=(VMEM,) * 4,
        cost_estimate=pl.CostEstimate(flops=2_000_000, bytes_accessed=2_000_000, transcendentals=0),
    )(near, far, taste_scale.reshape(1, K))
    d, n = lax.axis_index("draw"), lax.axis_index("nest")
    tastes = []
    for shift in range(4):
        to = (d + shift) % 4
        piece = lax.dynamic_slice_in_dim(taste_draws, to * 8 + n * QUAD, QUAD, 0)
        if shift:
            piece = lax.ppermute(piece, "draw", [(i, (i + shift) % 4) for i in range(4)])
        tastes.append(piece)

    big = (QUAD, len(PLACES), HALF, DRAWS)
    small = (QUAD, len(PLACES), HALF, LANES)
    results = pl.pallas_call(
        contract,
        name="contract",
        out_shape=jax.ShapeDtypeStruct((8, 32, LANES), f32),
        in_specs=[VMEM] * 9,
        out_specs=VMEM,
        scratch_shapes=[
            pltpu.VMEM((rows, LANES), bf16),
            pltpu.VMEM((QUAD, QUAD * K, DRAWS), bf16),
            pltpu.VMEM(big, f32),
            pltpu.VMEM(big, f32),
            pltpu.VMEM(small, f32),
            pltpu.VMEM(small, f32),
            pltpu.VMEM((BLOCKS * 8, LANES), f32),
        ],
        compiler_params=pltpu.CompilerParams(vmem_limit_bytes=40 * 1024 * 1024),
    )(recv, *tastes, *plan)
    gathered = lax.all_to_all(results, ("draw", "nest"), split_axis=0, concat_axis=0, tiled=True)
    shape = jax.ShapeDtypeStruct((32, HALF * SLOTS), f32)
    return pl.pallas_call(
        unpack, name="unpack", out_shape=(shape, shape), in_specs=[VMEM], out_specs=(VMEM, VMEM)
    )(gathered.reshape(256, LANES))


def solution(mesh):
    in_specs = (
        P(None, "mkt", None),
        P("mkt", None, "draw"),
        P(),
        P("nest"),
        P("nest", None),
        P("mkt", None),
    )
    out_specs = (P("mkt", "nest"), P("mkt", "nest"))
    return jax.shard_map(shards, mesh=mesh, in_specs=in_specs, out_specs=out_specs, check_vma=False)
```

```python
import math

import jax
import jax.numpy as jnp
from jax import lax
from jax.experimental import pallas as pl
from jax.experimental.pallas import tpu as pltpu
from jax.sharding import PartitionSpec as P


ITERS = 3
BLOCKS = 32
QUAD = 4
K = 32
PROD = 16
SLOTS = 48
NESTS = 16
HALF = 8
DRAWS = 512
MARKETS = 1024
LANES = 128
ROWS = 24
LOG2E = 1.0 / math.log(2.0)
LOW = -1e30
MIB = 1024 * 1024
TINY = 1.1754944e-38
EMPTY = 32 * 16 + 15
PLACES = [(o, t) for o in range(2) for t in range(SLOTS)]
f32, bf16, i32 = jnp.float32, jnp.bfloat16, jnp.int32
VMEM = pl.BlockSpec(memory_space=pltpu.VMEM)
HBM = pl.BlockSpec(memory_space=pltpu.HBM)
PARTS = 2


def iota(shape, dim):
    return lax.broadcasted_iota(i32, shape, dim)


def dot(a, b):
    return lax.dot_general(a, b, (((1,), (0,)), ((), ())), preferred_element_type=f32)


def dot_t(a, b):
    return lax.dot_general(a, b, (((1,), (1,)), ((), ())), preferred_element_type=f32)


def pack(f_hbm, l_hbm, out_hbm, f_ref, l_ref, g_ref, o_ref, s_ref, out_ref, sems):
    loads = [pltpu.make_async_copy(l_hbm, l_ref, sems.at[PARTS])]
    for c in range(PARTS):
        part = pl.ds(c * K // PARTS, K // PARTS)
        loads.append(pltpu.make_async_copy(f_hbm.at[part], f_ref.at[part], sems.at[c]))
    for load in loads:
        load.start()
    base = (lax.axis_index("draw") * 2 + lax.axis_index("nest")) * QUAD
    market = iota((MARKETS, LANES), 0)
    lane = iota((MARKETS, LANES), 1)
    pick = jnp.where(market == (lane % BLOCKS) * 32 + base + lane // BLOCKS, 1.0, 0.0).astype(bf16)
    spread = jnp.where(iota((BLOCKS, LANES), 0) == iota((BLOCKS, LANES), 1) % BLOCKS, 1.0, 0.0).astype(bf16)

    loads[0].wait()
    log = l_ref[...]
    high = log.astype(bf16)
    rest = log - high.astype(f32)
    middle = rest.astype(bf16)
    low = (rest - middle.astype(f32)).astype(bf16)
    logs = dot(jnp.concatenate([high, middle, low], axis=0), pick)
    own = (iota((LANES, LANES), 0) // PROD) % QUAD == iota((LANES, LANES), 1) // BLOCKS
    first = jnp.concatenate([logs[:PROD]] * QUAD + [logs[PROD : 2 * PROD]] * QUAD, axis=0)
    second = jnp.concatenate([logs[2 * PROD :]] * QUAD + [jnp.zeros((64, LANES), f32)], axis=0)
    s_ref[...] = jnp.zeros_like(s_ref)
    s_ref[pl.ds(0, BLOCKS, stride=8), :] = dot_t(spread, jnp.where(own, first, 0.0).astype(bf16))
    s_ref[pl.ds(1, BLOCKS, stride=8), :] = dot_t(spread, jnp.where(own, second, 0.0).astype(bf16))

    rows = K * PROD // PARTS
    for c in range(PARTS):
        loads[1 + c].wait()
        part = f_ref[c * K // PARTS : (c + 1) * K // PARTS].reshape(rows, MARKETS)
        g_ref[c * rows : (c + 1) * rows, :] = dot(part, pick)
    own = iota((LANES, LANES), 0) // K == iota((LANES, LANES), 1) // BLOCKS
    parts = []
    for j in range(PROD):
        part = g_ref[pl.ds(j, K, stride=PROD), :]
        parts.append(jnp.where(own, jnp.concatenate([part] * QUAD, axis=0), 0.0).astype(bf16))
    goods = dot_t(spread, jnp.concatenate(parts, axis=0))
    for j in range(PROD):
        o_ref[pl.ds(j, BLOCKS, stride=PROD), :] = goods[:, j * LANES : (j + 1) * LANES]
    stores = []
    for c in range(2):
        half = slice(c * BLOCKS // 2, (c + 1) * BLOCKS // 2)
        goods = o_ref[c * 256 : (c + 1) * 256, :].reshape(BLOCKS // 2, PROD, LANES)
        out_ref[half, :PROD, :] = goods.astype(bf16)
        logs = s_ref[c * 128 : (c + 1) * 128, :].reshape(BLOCKS // 2, 8, LANES)
        out_ref[half, PROD:, :] = logs.astype(bf16)
        half = pl.ds(c * BLOCKS // 2, BLOCKS // 2)
        stores.append(pltpu.make_async_copy(out_ref.at[half], out_hbm.at[half], sems.at[c]))
        stores[-1].start()
    for store in stores:
        store.wait()


def across(x):
    return jnp.concatenate([x] * (DRAWS // LANES), axis=1)


def arrange(near_ref, far_ref, scale_ref, table_ref, hot_ref, pick_ref, mask_ref):
    near, far = near_ref[...], far_ref[...]
    first = lax.axis_index("nest") == 0
    table = jnp.concatenate([jnp.where(first, near, far), jnp.where(first, far, near)], axis=0)
    table_ref[:NESTS, :] = table
    square = iota((K, K), 0) == iota((K, K), 1)
    scale = jnp.sum(jnp.where(square, jnp.broadcast_to(scale_ref[...], (K, K)), 0.0), axis=1, keepdims=True)
    table_ref[NESTS:, :] = jnp.broadcast_to(scale, (K, LANES))
    ids = table.astype(i32)
    ids = jnp.where(ids < 0, EMPTY, ids)
    wide, narrow = iota((HALF, DRAWS), 1), iota((HALF, LANES), 1)
    for b in range(0, len(PLACES), 2):
        hot, pick, mask = [], [], []
        for o, t in PLACES[b : b + 2]:
            here = jnp.broadcast_to(ids[o * HALF : (o + 1) * HALF, t : t + 1], (HALF, LANES))
            hot.append(jnp.where(across(here) == wide, 1.0, 0.0))
            pick.append(jnp.where((here >> 4) == narrow, 1.0, 0.0))
            mask.append(jnp.where((here & 15) == (narrow & 15), 1.0, 0.0))
        rows = slice(b * HALF, (b + 2) * HALF)
        hot_ref[rows, :] = jnp.concatenate(hot, axis=0).astype(bf16)
        pick_ref[rows, :] = jnp.concatenate(pick, axis=0).astype(bf16)
        mask_ref[rows, :] = jnp.concatenate(mask, axis=0).astype(bf16)


def contract(x_ref, t0_ref, t1_ref, t2_ref, t3_ref, table_ref, hot_ref, pick_ref, mask_ref, out_ref,
             slot_ref, taste_ref, mu_ref, e_ref, v_ref, t_ref, l_ref):
    table = [table_ref[o * HALF : (o + 1) * HALF, :] for o in range(2)]
    rate = [jnp.broadcast_to(x[:, SLOTS : SLOTS + 1], (HALF, LANES)) for x in table]
    inverse = [1.0 / x for x in rate]
    to_two = [across(LOG2E * x) for x in inverse]
    gain = [(1.0 - x) * y for x, y in zip(rate, inverse)]
    less = [across(x - 1.0) for x in rate]
    narrow = iota((HALF, LANES), 1)

    l_ref[...] = x_ref[:, PROD:, :].astype(f32).reshape(BLOCKS * 8, LANES)
    top = l_ref[pl.ds(0, BLOCKS, stride=8), :]
    rest = l_ref[pl.ds(1, BLOCKS, stride=8), :]
    both = jnp.concatenate([top, rest], axis=1)
    lane = iota((BLOCKS, 2 * LANES), 1)
    lows = (iota((BLOCKS, 2 * LANES), 0) == 0) & (lane < 64) & (lane % PROD == PROD - 1)
    both = jnp.concatenate([both, jnp.where(lows, LOW, 0.0), jnp.zeros((64, 2 * LANES), f32)], axis=0).astype(bf16)
    rows = dot(pick_ref[...], both).astype(bf16)
    mask = mask_ref[...]
    rows = rows * jnp.concatenate([mask, mask], axis=1)
    copies = jnp.where(
        (iota((2 * LANES, DRAWS), 0) // PROD) % QUAD == iota((2 * LANES, DRAWS), 1) // LANES, 1.0, 0.0
    ).astype(bf16)
    target = dot(rows, copies)
    whole = (top + pltpu.roll(top, 64, 1)) + rest
    shares = jnp.exp(whole)
    column = iota((BLOCKS, LANES), 1)
    outside = []
    for q in range(QUAD):
        inside = jnp.where(column // PROD == q, shares, 0.0)
        total = 1.0 - jnp.sum(jnp.sum(inside, axis=1, keepdims=True), axis=0, keepdims=True)
        outside.append(lax.log2(jnp.broadcast_to(total, (HALF, LANES))))

    x = x_ref[:, :PROD, :].reshape(BLOCKS * PROD, LANES)
    slot_ref[...] = dot(hot_ref[...], x).astype(bf16)
    scale = table_ref[NESTS:, :]
    taste_ref[...] = jnp.zeros_like(taste_ref)
    for q in range(QUAD):
        for b, ref in enumerate((t0_ref, t1_ref, t2_ref, t3_ref)):
            taste = (scale * ref[q].astype(f32)).astype(bf16)
            taste_ref[q, q * K : (q + 1) * K, b * LANES : (b + 1) * LANES] = taste

    def weights(inner):
        power = [jnp.exp2(x * lax.log2(y)) for x, y in zip(less, inner)]
        total = jnp.sum(power[0] * inner[0] + power[1] * inner[1], axis=0, keepdims=True)
        total = (1.0 + total) * DRAWS
        return [x / total for x in power]

    def first_half(q, b, inner, value, mu):
        o = PLACES[b][0]
        e = jnp.exp2(mu + across(value))
        e_ref[q, b] = e
        inner[o] = inner[o] + e

    def second_half(q, b, weight):
        o = PLACES[b][0]
        p = e_ref[q, b] * weight[o]
        p = (p[:, :128] + p[:, 128:256]) + (p[:, 256:384] + p[:, 384:])
        share = jnp.broadcast_to(jnp.sum(p, axis=1, keepdims=True), (HALF, LANES))
        value = v_ref[q, b] + gain[o] * (t_ref[q, b] - lax.log2(jnp.maximum(share, TINY)))
        return value, share

    zeros = jnp.zeros((HALF, DRAWS), f32)
    weight = [None] * QUAD
    count = len(PLACES)
    for q in range(QUAD):
        mu = dot(slot_ref[...], taste_ref[q])
        inner = [zeros, zeros]
        for b, (o, _) in enumerate(PLACES):
            part = mu[b * HALF : (b + 1) * HALF] * to_two[o]
            mu_ref[q, b] = part
            goal = target[b * HALF : (b + 1) * HALF, q * LANES : (q + 1) * LANES] * LOG2E
            t_ref[q, b] = goal
            value = (goal - outside[q]) * inverse[o]
            v_ref[q, b] = value
            first_half(q, b, inner, value, part)
        weight[q] = weights(inner)

    for _ in range(ITERS - 1):
        old = list(weight)
        for q in range(QUAD + 1):
            inner = [zeros, zeros]
            for b in range(count):
                if q < QUAD:
                    v_ref[q, b] = second_half(q, b, old[q])[0]
                if q:
                    first_half(q - 1, b, inner, v_ref[q - 1, b], mu_ref[q - 1, b])
            if q:
                weight[q - 1] = weights(inner)

    back = [x * math.log(2.0) for x in rate]
    for q in range(QUAD):
        values = [jnp.zeros((HALF, LANES), f32)] * 2
        shares = [jnp.zeros((HALF, LANES), f32)] * 2
        for b, (o, t) in enumerate(PLACES):
            value, share = second_half(q, b, weight[q])
            values[o] = jnp.where(narrow == t, value, values[o])
            shares[o] = jnp.where(narrow == t + 64, share, shares[o])
        for n in range(2):
            value = jnp.where(table[n] >= 0.0, values[n] * back[n], 0.0)
            both = jnp.where(narrow < SLOTS, value, shares[n])
            for d in range(4):
                out_ref[2 * d + n, q * HALF : (q + 1) * HALF, :] = both


def unpack(r_ref, value_ref, share_ref):
    for g in range(HALF):
        part = r_ref[pl.ds(g, 32, stride=HALF), :]
        value_ref[:, g * SLOTS : (g + 1) * SLOTS] = part[:, :SLOTS]
        share_ref[:, g * SLOTS : (g + 1) * SLOTS] = part[:, 64 : 64 + SLOTS]


def shards(features, taste_draws, taste_scale, nest_param, members, log_share):
    send = pl.pallas_call(
        pack,
        name="pack",
        out_shape=jax.ShapeDtypeStruct((BLOCKS, ROWS, LANES), bf16),
        in_specs=[HBM, HBM],
        out_specs=HBM,
        scratch_shapes=[
            pltpu.VMEM((K, PROD, MARKETS), bf16),
            pltpu.VMEM((PROD, MARKETS), f32),
            pltpu.VMEM((K * PROD, LANES), f32),
            pltpu.VMEM((BLOCKS * PROD, LANES), f32),
            pltpu.VMEM((BLOCKS * 8, LANES), f32),
            pltpu.VMEM((BLOCKS, ROWS, LANES), bf16),
            pltpu.SemaphoreType.DMA((PARTS + 1,)),
        ],
    )(features, log_share)
    recv = lax.all_to_all(send, "mkt", split_axis=0, concat_axis=0, tiled=True)

    near = jnp.concatenate(
        [members.astype(f32), nest_param[:, None], jnp.zeros((HALF, LANES - SLOTS - 1), f32)], axis=1
    )
    far = lax.ppermute(near, "nest", [(0, 1), (1, 0)])
    rows = len(PLACES) * HALF
    plan = pl.pallas_call(
        arrange,
        name="arrange",
        out_shape=(
            jax.ShapeDtypeStruct((NESTS + K, LANES), f32),
            jax.ShapeDtypeStruct((rows, DRAWS), bf16),
            jax.ShapeDtypeStruct((rows, LANES), bf16),
            jax.ShapeDtypeStruct((rows, LANES), bf16),
        ),
        in_specs=[VMEM] * 3,
        out_specs=(VMEM,) * 4,
        cost_estimate=pl.CostEstimate(flops=2_000_000, bytes_accessed=2_000_000, transcendentals=0),
        compiler_params=pltpu.CompilerParams(vmem_limit_bytes=4 * MIB),
    )(near, far, taste_scale.reshape(1, K))
    d, n = lax.axis_index("draw"), lax.axis_index("nest")
    tastes = []
    for shift in range(4):
        to = (d + shift) % 4
        piece = lax.dynamic_slice_in_dim(taste_draws, to * 8 + n * QUAD, QUAD, 0)
        if shift:
            piece = lax.ppermute(piece, "draw", [(i, (i + shift) % 4) for i in range(4)])
        tastes.append(piece)

    big = (QUAD, len(PLACES), HALF, DRAWS)
    small = (QUAD, len(PLACES), HALF, LANES)
    results = pl.pallas_call(
        contract,
        name="contract",
        out_shape=jax.ShapeDtypeStruct((8, 32, LANES), f32),
        in_specs=[VMEM] * 9,
        out_specs=VMEM,
        scratch_shapes=[
            pltpu.VMEM((rows, LANES), bf16),
            pltpu.VMEM((QUAD, QUAD * K, DRAWS), bf16),
            pltpu.VMEM(big, f32),
            pltpu.VMEM(big, f32),
            pltpu.VMEM(small, f32),
            pltpu.VMEM(small, f32),
            pltpu.VMEM((BLOCKS * 8, LANES), f32),
        ],
        compiler_params=pltpu.CompilerParams(vmem_limit_bytes=36 * MIB),
    )(recv, *tastes, *plan)
    gathered = lax.all_to_all(results, ("draw", "nest"), split_axis=0, concat_axis=0, tiled=True)
    shape = jax.ShapeDtypeStruct((32, HALF * SLOTS), f32)
    return pl.pallas_call(
        unpack,
        name="unpack",
        out_shape=(shape, shape),
        in_specs=[VMEM],
        out_specs=(VMEM, VMEM),
        compiler_params=pltpu.CompilerParams(vmem_limit_bytes=2 * MIB),
    )(gathered.reshape(256, LANES))


def solution(mesh):
    in_specs = (
        P(None, "mkt", None),
        P("mkt", None, "draw"),
        P(),
        P("nest"),
        P("nest", None),
        P("mkt", None),
    )
    out_specs = (P("mkt", "nest"), P("mkt", "nest"))


    return jax.shard_map(shards, mesh=mesh, in_specs=in_specs, out_specs=out_specs, check_vma=False)
```

```python
import math

import jax
import jax.numpy as jnp
from jax import lax
from jax.experimental import pallas as pl
from jax.experimental.pallas import tpu as pltpu
from jax.sharding import PartitionSpec as P


ITERS = 3
BLOCKS = 32
QUAD = 4
K = 32
PROD = 16
SLOTS = 48
NESTS = 16
HALF = 8
DRAWS = 512
MARKETS = 1024
LANES = 128
ROWS = 24
LOG2E = 1.0 / math.log(2.0)
LOW = -1e30
MIB = 1024 * 1024
TINY = 1.1754944e-38
EMPTY = 32 * 16 + 15
CUT = 32
PLACES = [(o, t) for t in range(CUT) for o in range(2)] + [(o, t) for o in range(2) for t in range(CUT, SLOTS)]
SHORT = len(PLACES) - (SLOTS - CUT)
f32, bf16, i32 = jnp.float32, jnp.bfloat16, jnp.int32
VMEM = pl.BlockSpec(memory_space=pltpu.VMEM)
HBM = pl.BlockSpec(memory_space=pltpu.HBM)
PARTS = 2


def iota(shape, dim):
    return lax.broadcasted_iota(i32, shape, dim)


def dot(a, b):
    return lax.dot_general(a, b, (((1,), (0,)), ((), ())), preferred_element_type=f32)


def dot_t(a, b):
    return lax.dot_general(a, b, (((1,), (1,)), ((), ())), preferred_element_type=f32)


def pack(f_hbm, l_hbm, out_hbm, f_ref, l_ref, g_ref, o_ref, s_ref, out_ref, sems):
    loads = [pltpu.make_async_copy(l_hbm, l_ref, sems.at[PARTS])]
    for c in range(PARTS):
        part = pl.ds(c * K // PARTS, K // PARTS)
        loads.append(pltpu.make_async_copy(f_hbm.at[part], f_ref.at[part], sems.at[c]))
    for load in loads:
        load.start()
    base = (lax.axis_index("draw") * 2 + lax.axis_index("nest")) * QUAD
    market = iota((MARKETS, LANES), 0)
    lane = iota((MARKETS, LANES), 1)
    pick = jnp.where(market == (lane % BLOCKS) * 32 + base + lane // BLOCKS, 1.0, 0.0).astype(bf16)
    spread = jnp.where(iota((BLOCKS, LANES), 0) == iota((BLOCKS, LANES), 1) % BLOCKS, 1.0, 0.0).astype(bf16)

    loads[0].wait()
    log = l_ref[...]
    high = log.astype(bf16)
    rest = log - high.astype(f32)
    middle = rest.astype(bf16)
    low = (rest - middle.astype(f32)).astype(bf16)
    logs = dot(jnp.concatenate([high, middle, low], axis=0), pick)
    own = (iota((LANES, LANES), 0) // PROD) % QUAD == iota((LANES, LANES), 1) // BLOCKS
    first = jnp.concatenate([logs[:PROD]] * QUAD + [logs[PROD : 2 * PROD]] * QUAD, axis=0)
    second = jnp.concatenate([logs[2 * PROD :]] * QUAD + [jnp.zeros((64, LANES), f32)], axis=0)
    s_ref[...] = jnp.zeros_like(s_ref)
    s_ref[pl.ds(0, BLOCKS, stride=8), :] = dot_t(spread, jnp.where(own, first, 0.0).astype(bf16))
    s_ref[pl.ds(1, BLOCKS, stride=8), :] = dot_t(spread, jnp.where(own, second, 0.0).astype(bf16))

    rows = K * PROD // PARTS
    for c in range(PARTS):
        loads[1 + c].wait()
        part = f_ref[c * K // PARTS : (c + 1) * K // PARTS].reshape(rows, MARKETS)
        g_ref[c * rows : (c + 1) * rows, :] = dot(part, pick)
    own = iota((LANES, LANES), 0) // K == iota((LANES, LANES), 1) // BLOCKS
    parts = []
    for j in range(PROD):
        part = g_ref[pl.ds(j, K, stride=PROD), :]
        parts.append(jnp.where(own, jnp.concatenate([part] * QUAD, axis=0), 0.0).astype(bf16))
    goods = dot_t(spread, jnp.concatenate(parts, axis=0))
    for j in range(PROD):
        o_ref[pl.ds(j, BLOCKS, stride=PROD), :] = goods[:, j * LANES : (j + 1) * LANES]
    stores = []
    for c in range(2):
        half = slice(c * BLOCKS // 2, (c + 1) * BLOCKS // 2)
        goods = o_ref[c * 256 : (c + 1) * 256, :].reshape(BLOCKS // 2, PROD, LANES)
        out_ref[half, :PROD, :] = goods.astype(bf16)
        logs = s_ref[c * 128 : (c + 1) * 128, :].reshape(BLOCKS // 2, 8, LANES)
        out_ref[half, PROD:, :] = logs.astype(bf16)
        half = pl.ds(c * BLOCKS // 2, BLOCKS // 2)
        stores.append(pltpu.make_async_copy(out_ref.at[half], out_hbm.at[half], sems.at[c]))
        stores[-1].start()
    for store in stores:
        store.wait()


def across(x):
    return jnp.concatenate([x] * (DRAWS // LANES), axis=1)


def arrange(near_ref, far_ref, scale_ref, table_ref, hot_ref, pick_ref, mask_ref):
    near, far = near_ref[...], far_ref[...]
    first = lax.axis_index("nest") == 0
    table = jnp.concatenate([jnp.where(first, near, far), jnp.where(first, far, near)], axis=0)
    row, lane = iota((NESTS, LANES), 0), iota((NESTS, LANES), 1)
    filled = jnp.where((lane < SLOTS) & (table >= 0.0), 1.0, 0.0)
    size = jnp.broadcast_to(jnp.sum(filled, axis=1, keepdims=True), (NESTS, LANES))
    across_size = jnp.sum(jnp.where(row == lane, size, 0.0), axis=0, keepdims=True)
    ahead = (across_size > size) | ((across_size == size) & (lane < row))
    ahead = jnp.where(ahead & (lane < NESTS), 1.0, 0.0)
    rank = jnp.broadcast_to(jnp.sum(ahead, axis=1, keepdims=True), (NESTS, LANES))
    across_rank = jnp.sum(jnp.where(row == lane, rank, 0.0), axis=0, keepdims=True)
    place = jnp.where((across_rank == row.astype(f32)) & (lane < NESTS), 1.0, 0.0)
    ordered = table
    for g in range(NESTS):
        chosen = jnp.broadcast_to(place[:, g : g + 1], (NESTS, LANES)) > 0.5
        ordered = jnp.where(chosen, jnp.broadcast_to(table[g : g + 1, :], (NESTS, LANES)), ordered)
    table = ordered
    table_ref[:NESTS, :] = table
    table_ref[NESTS + K :, :] = rank
    square = iota((K, K), 0) == iota((K, K), 1)
    scale = jnp.sum(jnp.where(square, jnp.broadcast_to(scale_ref[...], (K, K)), 0.0), axis=1, keepdims=True)
    table_ref[NESTS : NESTS + K, :] = jnp.broadcast_to(scale, (K, LANES))
    ids = table.astype(i32)
    ids = jnp.where(ids < 0, EMPTY, ids)
    wide, narrow = iota((HALF, DRAWS), 1), iota((HALF, LANES), 1)
    for b in range(0, len(PLACES), 2):
        hot, pick, mask = [], [], []
        for o, t in PLACES[b : b + 2]:
            here = jnp.broadcast_to(ids[o * HALF : (o + 1) * HALF, t : t + 1], (HALF, LANES))
            hot.append(jnp.where(across(here) == wide, 1.0, 0.0))
            pick.append(jnp.where((here >> 4) == narrow, 1.0, 0.0))
            mask.append(jnp.where((here & 15) == (narrow & 15), 1.0, 0.0))
        rows = slice(b * HALF, (b + 2) * HALF)
        hot_ref[rows, :] = jnp.concatenate(hot, axis=0).astype(bf16)
        pick_ref[rows, :] = jnp.concatenate(pick, axis=0).astype(bf16)
        mask_ref[rows, :] = jnp.concatenate(mask, axis=0).astype(bf16)


def solve(count, x_ref, taste_refs, table_ref, hot_ref, pick_ref, mask_ref, out_ref, slot_ref, taste_ref, l_ref):
    used = count * HALF
    table = [table_ref[o * HALF : (o + 1) * HALF, :] for o in range(2)]
    rate = [jnp.broadcast_to(x[:, SLOTS : SLOTS + 1], (HALF, LANES)) for x in table]
    inverse = [1.0 / x for x in rate]
    to_two = [across(LOG2E * x) for x in inverse]
    gain = [(1.0 - x) * y[:, :LANES] for x, y in zip(rate, to_two)]
    less = [across((x - 1.0) * LOG2E) for x in rate]
    narrow = iota((HALF, LANES), 1)

    l_ref[...] = x_ref[:, PROD:, :].astype(f32).reshape(BLOCKS * 8, LANES)
    top = l_ref[pl.ds(0, BLOCKS, stride=8), :]
    rest = l_ref[pl.ds(1, BLOCKS, stride=8), :]
    both = jnp.concatenate([top, rest], axis=1)
    lane = iota((BLOCKS, 2 * LANES), 1)
    lows = (iota((BLOCKS, 2 * LANES), 0) == 0) & (lane < 64) & (lane % PROD == PROD - 1)
    both = jnp.concatenate([both, jnp.where(lows, LOW, 0.0), jnp.zeros((64, 2 * LANES), f32)], axis=0).astype(bf16)
    rows = dot(pick_ref[:used, :], both).astype(bf16)
    mask = mask_ref[:used, :]
    rows = rows * jnp.concatenate([mask, mask], axis=1)
    source, lane = iota((2 * LANES, LANES), 0), iota((2 * LANES, LANES), 1)
    fold = jnp.where((source // 64) * QUAD + (source // PROD) % QUAD == lane, 1.0, 0.0).astype(bf16)
    parts = dot(rows, fold)
    ones = jnp.where((narrow >= 3 * QUAD) & (narrow < 3 * QUAD + 3), 1.0, 0.0)
    slot_ref[:used, LANES:] = (parts + jnp.concatenate([ones] * count, axis=0)).astype(bf16)
    copies = jnp.where((source // PROD) % QUAD == lane // 32, 1.0, 0.0).astype(bf16)
    goals = dot(rows, copies)
    whole = (top + pltpu.roll(top, 64, 1)) + rest
    shares = jnp.exp(whole)
    column = iota((BLOCKS, LANES), 1)
    outside = []
    for q in range(QUAD):
        inside = jnp.where(column // PROD == q, shares, 0.0)
        total = 1.0 - jnp.sum(jnp.sum(inside, axis=1, keepdims=True), axis=0, keepdims=True)
        outside.append(jnp.log(jnp.broadcast_to(total, (NESTS, LANES))))

    x = x_ref[:, :PROD, :].reshape(BLOCKS * PROD, LANES)
    slot_ref[:used, :LANES] = dot(hot_ref[:used, :], x).astype(bf16)
    scale = table_ref[NESTS : NESTS + K, :]
    taste_ref[...] = jnp.zeros_like(taste_ref)
    for q in range(QUAD):
        for b, ref in enumerate(taste_refs):
            taste = (scale * ref[q].astype(f32)).astype(bf16)
            taste_ref[q, q * K : (q + 1) * K, b * LANES : (b + 1) * LANES] = taste
        row = iota((NESTS, LANES), 0)
        start = jnp.where((row < 3 * QUAD) & (row % QUAD == q), 1.0, 0.0)
        rest = -outside[q]
        for part in range(3):
            piece = rest.astype(bf16).astype(f32)
            start = jnp.where(row == 3 * QUAD + part, piece, start)
            rest = rest - piece
        taste_ref[q, LANES : LANES + NESTS, :] = across(start).astype(bf16)

    def weights(inner):
        power = [jnp.exp2(x * jnp.log(y)) for x, y in zip(less, inner)]
        total = jnp.sum(power[0] * inner[0] + power[1] * inner[1], axis=0, keepdims=True)
        total = (1.0 + total) * DRAWS
        return [x / total for x in power]

    def exps(q, b, inner, power):
        o = PLACES[b][0]
        e = jnp.exp2(power)
        held[q, b] = e
        inner[o] = inner[o] + e

    def collect(b, tiles, copies):
        o, t = PLACES[b]
        tiles[o] = jnp.where(narrow == t, copies, tiles[o])

    def sums(q, b, weight, share):
        p = held[q, b] * weight[PLACES[b][0]]
        p = (p[:, :128] + p[:, 128:256]) + (p[:, 256:384] + p[:, 384:])
        collect(b, share, jnp.broadcast_to(jnp.sum(p, axis=1, keepdims=True), (HALF, LANES)))

    zeros = jnp.zeros((HALF, DRAWS), f32)
    held, base = {}, {}
    blank = jnp.zeros((HALF, LANES), f32)
    weight, target, value, share = [[None] * QUAD for _ in range(4)]
    for q in range(QUAD):
        mu = dot(slot_ref[:used, :], taste_ref[q])
        inner = [zeros, zeros]
        for b, (o, _) in enumerate(PLACES[:count]):
            part = mu[b * HALF : (b + 1) * HALF] * to_two[o]
            base[q, b] = part
            exps(q, b, inner, part)
        weight[q] = weights(inner)
        value[q] = [blank, blank]

    tiles = [[blank, blank], [blank, blank]]
    for b, (o, t) in enumerate(PLACES[:count]):
        tile = tiles[t // 32]
        tile[o] = jnp.where(narrow % 32 == t % 32, goals[b * HALF : (b + 1) * HALF], tile[o])
    for q in range(QUAD):
        target[q] = [
            jnp.where(narrow < 32, pltpu.roll(x, (128 - 32 * q) % 128, 1), pltpu.roll(y, (160 - 32 * q) % 128, 1))
            for x, y in zip(*tiles)
        ]

    lag = 2
    for stage in range(ITERS * QUAD):
        q = stage % QUAD
        ahead = stage - lag if 0 <= stage - lag < (ITERS - 1) * QUAD else None
        share[q], inner = [blank, blank], [zeros, zeros]
        for b in range(count):
            sums(q, b, weight[q], share[q])
            if ahead is not None:
                o, t = PLACES[b]
                move = jnp.broadcast_to(value[ahead % QUAD][o][:, t : t + 1], (HALF, LANES))
                exps(ahead % QUAD, b, inner, base[ahead % QUAD, b] + across(move))
        if ahead is not None:
            weight[ahead % QUAD] = weights(inner)
        value[q] = [
            v + g * (x - jnp.log(jnp.maximum(y, TINY))) for v, g, x, y in zip(value[q], gain, target[q], share[q])
        ]

    ranks = table_ref[NESTS + K :, :]
    for q in range(QUAD):
        final = jnp.zeros((NESTS, LANES), f32)
        for o in range(2):
            result = (target[q][o] - outside[q][:HALF]) + value[q][o] * (rate[o] * math.log(2.0))
            result = jnp.where(table[o] >= 0.0, result, 0.0)
            result = jnp.where(narrow < SLOTS, result, pltpu.roll(share[q][o], 64, 1))
            for r in range(HALF):
                one = jnp.broadcast_to(result[r : r + 1, :], (NESTS, LANES))
                final = jnp.where(ranks == float(o * HALF + r), one, final)
        for n in range(2):
            for d in range(4):
                out_ref[2 * d + n, q * HALF : (q + 1) * HALF, :] = final[n * HALF : (n + 1) * HALF]


def contract(x_ref, t0_ref, t1_ref, t2_ref, t3_ref, table_ref, hot_ref, pick_ref, mask_ref, out_ref,
             slot_ref, taste_ref, l_ref):
    inputs = (x_ref, (t0_ref, t1_ref, t2_ref, t3_ref), table_ref, hot_ref, pick_ref, mask_ref, out_ref)
    short = table_ref[HALF, CUT] < 0.0

    @pl.when(short)
    def _():
        solve(SHORT, *inputs, slot_ref, taste_ref, l_ref)

    @pl.when(jnp.logical_not(short))
    def _():
        solve(len(PLACES), *inputs, slot_ref, taste_ref, l_ref)


def unpack(r_ref, value_ref, share_ref):
    for g in range(HALF):
        part = r_ref[pl.ds(g, 32, stride=HALF), :]
        value_ref[:, g * SLOTS : (g + 1) * SLOTS] = part[:, :SLOTS]
        share_ref[:, g * SLOTS : (g + 1) * SLOTS] = part[:, 64 : 64 + SLOTS]


def shards(features, taste_draws, taste_scale, nest_param, members, log_share):
    send = pl.pallas_call(
        pack,
        name="pack",
        out_shape=jax.ShapeDtypeStruct((BLOCKS, ROWS, LANES), bf16),
        in_specs=[HBM, HBM],
        out_specs=HBM,
        scratch_shapes=[
            pltpu.VMEM((K, PROD, MARKETS), bf16),
            pltpu.VMEM((PROD, MARKETS), f32),
            pltpu.VMEM((K * PROD, LANES), f32),
            pltpu.VMEM((BLOCKS * PROD, LANES), f32),
            pltpu.VMEM((BLOCKS * 8, LANES), f32),
            pltpu.VMEM((BLOCKS, ROWS, LANES), bf16),
            pltpu.SemaphoreType.DMA((PARTS + 1,)),
        ],
    )(features, log_share)
    recv = lax.all_to_all(send, "mkt", split_axis=0, concat_axis=0, tiled=True)

    near = jnp.concatenate(
        [members.astype(f32), nest_param[:, None], jnp.zeros((HALF, LANES - SLOTS - 1), f32)], axis=1
    )
    far = lax.ppermute(near, "nest", [(0, 1), (1, 0)])
    rows = len(PLACES) * HALF
    plan = pl.pallas_call(
        arrange,
        name="arrange",
        out_shape=(
            jax.ShapeDtypeStruct((NESTS + K + NESTS, LANES), f32),
            jax.ShapeDtypeStruct((rows, DRAWS), bf16),
            jax.ShapeDtypeStruct((rows, LANES), bf16),
            jax.ShapeDtypeStruct((rows, LANES), bf16),
        ),
        in_specs=[VMEM] * 3,
        out_specs=(VMEM,) * 4,
        cost_estimate=pl.CostEstimate(flops=2_000_000, bytes_accessed=2_000_000, transcendentals=0),
        compiler_params=pltpu.CompilerParams(vmem_limit_bytes=4 * MIB),
    )(near, far, taste_scale.reshape(1, K))
    d, n = lax.axis_index("draw"), lax.axis_index("nest")
    tastes = []
    for shift in range(4):
        to = (d + shift) % 4
        piece = lax.dynamic_slice_in_dim(taste_draws, to * 8 + n * QUAD, QUAD, 0)
        if shift:
            piece = lax.ppermute(piece, "draw", [(i, (i + shift) % 4) for i in range(4)])
        tastes.append(piece)

    results = pl.pallas_call(
        contract,
        name="contract",
        out_shape=jax.ShapeDtypeStruct((8, 32, LANES), f32),
        in_specs=[VMEM] * 9,
        out_specs=VMEM,
        scratch_shapes=[
            pltpu.VMEM((rows, 2 * LANES), bf16),
            pltpu.VMEM((QUAD, 2 * LANES, DRAWS), bf16),
            pltpu.VMEM((BLOCKS * 8, LANES), f32),
        ],
        compiler_params=pltpu.CompilerParams(vmem_limit_bytes=36 * MIB),
    )(recv, *tastes, *plan)
    gathered = lax.all_to_all(results, ("draw", "nest"), split_axis=0, concat_axis=0, tiled=True)
    shape = jax.ShapeDtypeStruct((32, HALF * SLOTS), f32)
    return pl.pallas_call(
        unpack,
        name="unpack",
        out_shape=(shape, shape),
        in_specs=[VMEM],
        out_specs=(VMEM, VMEM),
        compiler_params=pltpu.CompilerParams(vmem_limit_bytes=2 * MIB),
    )(gathered.reshape(256, LANES))


def solution(mesh):
    in_specs = (
        P(None, "mkt", None),
        P("mkt", None, "draw"),
        P(),
        P("nest"),
        P("nest", None),
        P("mkt", None),
    )
    out_specs = (P("mkt", "nest"), P("mkt", "nest"))


    return jax.shard_map(shards, mesh=mesh, in_specs=in_specs, out_specs=out_specs, check_vma=False)
```

```python
import math

import jax
import jax.numpy as jnp
from jax import lax
from jax.experimental import pallas as pl
from jax.experimental.pallas import tpu as pltpu
from jax.sharding import PartitionSpec as P


ITERS = 3
BLOCKS = 32
QUAD = 4
K = 32
PROD = 16
SLOTS = 48
NESTS = 16
HALF = 8
DRAWS = 512
MARKETS = 1024
LANES = 128
ROWS = 18
LOG2E = 1.0 / math.log(2.0)
LOW = -1e30
MIB = 1024 * 1024
TINY = 1.1754944e-38
EMPTY = 32 * 16 + 15
CUT = 32
PLACES = [(o, t) for t in range(CUT) for o in range(2)] + [(o, t) for o in range(2) for t in range(CUT, SLOTS)]
SHORT = len(PLACES) - (SLOTS - CUT)
f32, bf16, i32 = jnp.float32, jnp.bfloat16, jnp.int32
VMEM = pl.BlockSpec(memory_space=pltpu.VMEM)
HBM = pl.BlockSpec(memory_space=pltpu.HBM)
PARTS = 2


def iota(shape, dim):
    return lax.broadcasted_iota(i32, shape, dim)


def dot(a, b):
    return lax.dot_general(a, b, (((1,), (0,)), ((), ())), preferred_element_type=f32)


def dot_t(a, b):
    return lax.dot_general(a, b, (((1,), (1,)), ((), ())), preferred_element_type=f32)


def pack(f_hbm, l_hbm, out_hbm, f_ref, l_ref, g_ref, o_ref, out_ref, sems):
    loads = [pltpu.make_async_copy(l_hbm, l_ref, sems.at[PARTS])]
    for c in range(PARTS):
        part = pl.ds(c * K // PARTS, K // PARTS)
        loads.append(pltpu.make_async_copy(f_hbm.at[part], f_ref.at[part], sems.at[c]))
    for load in loads:
        load.start()
    base = (lax.axis_index("draw") * 2 + lax.axis_index("nest")) * QUAD
    market = iota((MARKETS, LANES), 0)
    lane = iota((MARKETS, LANES), 1)
    pick = jnp.where(market == (lane % BLOCKS) * 32 + base + lane // BLOCKS, 1.0, 0.0).astype(bf16)
    spread = jnp.where(iota((BLOCKS, LANES), 0) == iota((BLOCKS, LANES), 1) % BLOCKS, 1.0, 0.0).astype(bf16)

    loads[0].wait()
    log = l_ref[...]
    high = log.astype(bf16)
    rest = log - high.astype(f32)
    middle = rest.astype(bf16)
    low = (rest - middle.astype(f32)).astype(bf16)
    logs = dot(jnp.concatenate([high, middle, low], axis=0), pick)
    own = (iota((LANES, LANES), 0) // PROD) % QUAD == iota((LANES, LANES), 1) // BLOCKS
    first = jnp.concatenate([logs[:PROD]] * QUAD + [logs[PROD : 2 * PROD]] * QUAD, axis=0)
    second = jnp.concatenate([logs[2 * PROD :]] * QUAD + [jnp.zeros((64, LANES), f32)], axis=0)
    o_ref[pl.ds(PROD, BLOCKS, stride=ROWS), :] = dot_t(spread, jnp.where(own, first, 0.0).astype(bf16))
    o_ref[pl.ds(PROD + 1, BLOCKS, stride=ROWS), :] = dot_t(spread, jnp.where(own, second, 0.0).astype(bf16))

    rows = K * PROD // PARTS
    for c in range(PARTS):
        loads[1 + c].wait()
        part = f_ref[c * K // PARTS : (c + 1) * K // PARTS].reshape(rows, MARKETS)
        g_ref[c * rows : (c + 1) * rows, :] = dot(part, pick)
    own = iota((LANES, LANES), 0) // K == iota((LANES, LANES), 1) // BLOCKS
    parts = []
    for j in range(PROD):
        part = g_ref[pl.ds(j, K, stride=PROD), :]
        parts.append(jnp.where(own, jnp.concatenate([part] * QUAD, axis=0), 0.0).astype(bf16))
    goods = dot_t(spread, jnp.concatenate(parts, axis=0))
    for j in range(PROD):
        o_ref[pl.ds(j, BLOCKS, stride=ROWS), :] = goods[:, j * LANES : (j + 1) * LANES]
    stores = []
    half = BLOCKS * ROWS // 2
    for c in range(2):
        out_ref[c * half : (c + 1) * half, :] = o_ref[c * half : (c + 1) * half, :].astype(bf16)
        part = pl.ds(c * half, half)
        stores.append(pltpu.make_async_copy(out_ref.at[part], out_hbm.at[part], sems.at[c]))
        stores[-1].start()
    for store in stores:
        store.wait()


def across(x):
    return jnp.concatenate([x] * (DRAWS // LANES), axis=1)


def arrange(near_ref, next_ref, scale_ref, table_ref, hot_ref, pick_ref, mask_ref):
    first = lax.axis_index("nest") == 0
    near, far = near_ref[...], next_ref[QUAD * K :, :]
    table = jnp.concatenate([jnp.where(first, near, far), jnp.where(first, far, near)], axis=0)
    row, lane = iota((NESTS, LANES), 0), iota((NESTS, LANES), 1)
    filled = jnp.where((lane < SLOTS) & (table >= 0.0), 1.0, 0.0)
    size = jnp.broadcast_to(jnp.sum(filled, axis=1, keepdims=True), (NESTS, LANES))
    across_size = jnp.sum(jnp.where(row == lane, size, 0.0), axis=0, keepdims=True)
    ahead = (across_size > size) | ((across_size == size) & (lane < row))
    ahead = jnp.where(ahead & (lane < NESTS), 1.0, 0.0)
    rank = jnp.broadcast_to(jnp.sum(ahead, axis=1, keepdims=True), (NESTS, LANES))
    across_rank = jnp.sum(jnp.where(row == lane, rank, 0.0), axis=0, keepdims=True)
    place = jnp.where((across_rank == row.astype(f32)) & (lane < NESTS), 1.0, 0.0)
    ordered = table
    for g in range(NESTS):
        chosen = jnp.broadcast_to(place[:, g : g + 1], (NESTS, LANES)) > 0.5
        ordered = jnp.where(chosen, jnp.broadcast_to(table[g : g + 1, :], (NESTS, LANES)), ordered)
    table = ordered
    table_ref[:NESTS, :] = table
    table_ref[NESTS + K :, :] = rank
    square = iota((K, K), 0) == iota((K, K), 1)
    scale = jnp.sum(jnp.where(square, jnp.broadcast_to(scale_ref[...], (K, K)), 0.0), axis=1, keepdims=True)
    table_ref[NESTS : NESTS + K, :] = jnp.broadcast_to(scale, (K, LANES))
    ids = table.astype(i32)
    ids = jnp.where(ids < 0, EMPTY, ids)
    wide, narrow = iota((HALF, DRAWS), 1), iota((HALF, LANES), 1)
    for b in range(0, len(PLACES), 2):
        hot, pick, mask = [], [], []
        for o, t in PLACES[b : b + 2]:
            here = jnp.broadcast_to(ids[o * HALF : (o + 1) * HALF, t : t + 1], (HALF, LANES))
            hot.append(jnp.where(across(here) == wide, 1.0, 0.0))
            pick.append(jnp.where((here >> 4) == narrow, 1.0, 0.0))
            mask.append(jnp.where((here & 15) == (narrow & 15), 1.0, 0.0))
        rows = slice(b * HALF, (b + 2) * HALF)
        hot_ref[rows, :] = jnp.concatenate(hot, axis=0).astype(bf16)
        pick_ref[rows, :] = jnp.concatenate(pick, axis=0).astype(bf16)
        mask_ref[rows, :] = jnp.concatenate(mask, axis=0).astype(bf16)


def solve(count, x_ref, taste_refs, table_ref, hot_ref, pick_ref, mask_ref, out_ref, slot_ref, taste_ref, l_ref):
    used = count * HALF
    table = [table_ref[o * HALF : (o + 1) * HALF, :] for o in range(2)]
    rate = [jnp.broadcast_to(x[:, SLOTS : SLOTS + 1], (HALF, LANES)) for x in table]
    inverse = [1.0 / x for x in rate]
    to_two = [across(LOG2E * x) for x in inverse]
    gain = [(1.0 - x) * y[:, :LANES] for x, y in zip(rate, to_two)]
    less = [across((x - 1.0) * LOG2E) for x in rate]
    narrow = iota((HALF, LANES), 1)

    l_ref[...] = x_ref[...].astype(f32)
    top = l_ref[pl.ds(PROD, BLOCKS, stride=ROWS), :]
    rest = l_ref[pl.ds(PROD + 1, BLOCKS, stride=ROWS), :]
    both = jnp.concatenate([top, rest], axis=1)
    lane = iota((BLOCKS, 2 * LANES), 1)
    lows = (iota((BLOCKS, 2 * LANES), 0) == 0) & (lane < 64) & (lane % PROD == PROD - 1)
    both = jnp.concatenate([both, jnp.where(lows, LOW, 0.0), jnp.zeros((64, 2 * LANES), f32)], axis=0).astype(bf16)
    rows = dot(pick_ref[:used, :], both).astype(bf16)
    mask = mask_ref[:used, :]
    rows = rows * jnp.concatenate([mask, mask], axis=1)
    source, lane = iota((2 * LANES, 2 * LANES), 0), iota((2 * LANES, 2 * LANES), 1)
    market = (source // PROD) % QUAD
    fold = ((lane < LANES) & ((source // 64) * QUAD + market == lane)) | ((lane >= LANES) & (market == lane // 32 - QUAD))
    folded = dot(rows, jnp.where(fold, 1.0, 0.0).astype(bf16))
    goals = folded[:, LANES:]
    ones = jnp.where((narrow >= 3 * QUAD) & (narrow < 3 * QUAD + 3), 1.0, 0.0)
    slot_ref[:used, LANES:] = (folded[:, :LANES] + jnp.concatenate([ones] * count, axis=0)).astype(bf16)
    whole = (top + pltpu.roll(top, 64, 1)) + rest
    shares = jnp.exp(whole)
    column = iota((BLOCKS, LANES), 1)
    outside = []
    for q in range(QUAD):
        inside = jnp.where(column // PROD == q, shares, 0.0)
        total = 1.0 - jnp.sum(jnp.sum(inside, axis=1, keepdims=True), axis=0, keepdims=True)
        outside.append(jnp.log(jnp.broadcast_to(total, (NESTS, LANES))))

    x = jnp.concatenate([l_ref[i * ROWS : i * ROWS + PROD, :] for i in range(BLOCKS)], axis=0).astype(bf16)
    slot_ref[:used, :LANES] = dot(hot_ref[:used, :], x).astype(bf16)
    scale = table_ref[NESTS : NESTS + K, :]
    taste_ref[...] = jnp.zeros_like(taste_ref)
    for q in range(QUAD):
        for b, ref in enumerate(taste_refs):
            taste = ref[q] if b != 1 else ref[q * K : (q + 1) * K, :]
            taste = (scale * taste.astype(f32)).astype(bf16)
            taste_ref[q, q * K : (q + 1) * K, b * LANES : (b + 1) * LANES] = taste
        row = iota((NESTS, LANES), 0)
        start = jnp.where((row < 3 * QUAD) & (row % QUAD == q), 1.0, 0.0)
        rest = -outside[q]
        for part in range(3):
            piece = rest.astype(bf16).astype(f32)
            start = jnp.where(row == 3 * QUAD + part, piece, start)
            rest = rest - piece
        taste_ref[q, LANES : LANES + NESTS, :] = across(start).astype(bf16)

    def weights(inner):
        power = [jnp.exp2(x * jnp.log(y)) for x, y in zip(less, inner)]
        total = jnp.sum(power[0] * inner[0] + power[1] * inner[1], axis=0, keepdims=True)
        total = (1.0 + total) * DRAWS
        return [x / total for x in power]

    def exps(q, b, inner, power):
        o = PLACES[b][0]
        e = jnp.exp2(power)
        held[q, b] = e
        inner[o] = inner[o] + e

    def collect(b, tiles, copies):
        o, t = PLACES[b]
        tiles[o] = jnp.where(narrow == t, copies, tiles[o])

    def sums(q, b, weight, share):
        p = held[q, b] * weight[PLACES[b][0]]
        p = (p[:, :128] + p[:, 128:256]) + (p[:, 256:384] + p[:, 384:])
        collect(b, share, jnp.broadcast_to(jnp.sum(p, axis=1, keepdims=True), (HALF, LANES)))

    zeros = jnp.zeros((HALF, DRAWS), f32)
    held, base = {}, {}
    blank = jnp.zeros((HALF, LANES), f32)
    weight, target, value, share = [[None] * QUAD for _ in range(4)]
    for q in range(QUAD):
        mu = dot(slot_ref[:used, :], taste_ref[q])
        inner = [zeros, zeros]
        for b, (o, _) in enumerate(PLACES[:count]):
            part = mu[b * HALF : (b + 1) * HALF] * to_two[o]
            base[q, b] = part
            exps(q, b, inner, part)
        weight[q] = weights(inner)
        value[q] = [blank, blank]

    tiles = [[blank, blank], [blank, blank]]
    for b, (o, t) in enumerate(PLACES[:count]):
        tile = tiles[t // 32]
        tile[o] = jnp.where(narrow % 32 == t % 32, goals[b * HALF : (b + 1) * HALF], tile[o])
    for q in range(QUAD):
        target[q] = [
            jnp.where(narrow < 32, pltpu.roll(x, (128 - 32 * q) % 128, 1), pltpu.roll(y, (160 - 32 * q) % 128, 1))
            for x, y in zip(*tiles)
        ]

    lag = 2
    for stage in range(ITERS * QUAD):
        q = stage % QUAD
        ahead = stage - lag if 0 <= stage - lag < (ITERS - 1) * QUAD else None
        share[q], inner = [blank, blank], [zeros, zeros]
        for b in range(count):
            sums(q, b, weight[q], share[q])
            if ahead is not None:
                o, t = PLACES[b]
                move = jnp.broadcast_to(value[ahead % QUAD][o][:, t : t + 1], (HALF, LANES))
                exps(ahead % QUAD, b, inner, base[ahead % QUAD, b] + across(move))
        if ahead is not None:
            weight[ahead % QUAD] = weights(inner)
        value[q] = [
            v + g * (x - jnp.log(jnp.maximum(y, TINY))) for v, g, x, y in zip(value[q], gain, target[q], share[q])
        ]

    ranks = table_ref[NESTS + K :, :]
    for q in range(QUAD):
        final = jnp.zeros((NESTS, LANES), f32)
        for o in range(2):
            result = (target[q][o] - outside[q][:HALF]) + value[q][o] * (rate[o] * math.log(2.0))
            result = jnp.where(table[o] >= 0.0, result, 0.0)
            result = jnp.where(narrow < SLOTS, result, pltpu.roll(share[q][o], 64, 1))
            for r in range(HALF):
                one = jnp.broadcast_to(result[r : r + 1, :], (NESTS, LANES))
                final = jnp.where(ranks == float(o * HALF + r), one, final)
        for n in range(2):
            for d in range(4):
                out_ref[2 * d + n, q * HALF : (q + 1) * HALF, :] = final[n * HALF : (n + 1) * HALF]


def contract(x_ref, t0_ref, t1_ref, t2_ref, t3_ref, table_ref, hot_ref, pick_ref, mask_ref, out_ref,
             slot_ref, taste_ref, l_ref):
    inputs = (x_ref, (t0_ref, t1_ref, t2_ref, t3_ref), table_ref, hot_ref, pick_ref, mask_ref, out_ref)
    short = table_ref[HALF, CUT] < 0.0

    @pl.when(short)
    def _():
        solve(SHORT, *inputs, slot_ref, taste_ref, l_ref)

    @pl.when(jnp.logical_not(short))
    def _():
        solve(len(PLACES), *inputs, slot_ref, taste_ref, l_ref)


def unpack(r_ref, value_ref, share_ref):
    for g in range(HALF):
        part = r_ref[pl.ds(g, 32, stride=HALF), :]
        value_ref[:, g * SLOTS : (g + 1) * SLOTS] = part[:, :SLOTS]
        share_ref[:, g * SLOTS : (g + 1) * SLOTS] = part[:, 64 : 64 + SLOTS]


def shards(features, taste_draws, taste_scale, nest_param, members, log_share):
    send = pl.pallas_call(
        pack,
        name="pack",
        out_shape=jax.ShapeDtypeStruct((BLOCKS * ROWS, LANES), bf16),
        in_specs=[HBM, HBM],
        out_specs=HBM,
        scratch_shapes=[
            pltpu.VMEM((K, PROD, MARKETS), bf16),
            pltpu.VMEM((PROD, MARKETS), f32),
            pltpu.VMEM((K * PROD, LANES), f32),
            pltpu.VMEM((BLOCKS * ROWS, LANES), f32),
            pltpu.VMEM((BLOCKS * ROWS, LANES), bf16),
            pltpu.SemaphoreType.DMA((PARTS + 1,)),
        ],
    )(features, log_share)
    send = send.reshape(BLOCKS, ROWS // 2, 2, LANES)
    recv = lax.all_to_all(send, "mkt", split_axis=0, concat_axis=0, tiled=True)
    recv = recv.reshape(BLOCKS * ROWS, LANES)

    d, n = lax.axis_index("draw"), lax.axis_index("nest")

    def tastes(shift, nest):
        return lax.dynamic_slice_in_dim(taste_draws, (d + shift) % 4 * 8 + nest * QUAD, QUAD, 0)

    near = jnp.concatenate(
        [members.astype(f32), nest_param[:, None], jnp.zeros((HALF, LANES - SLOTS - 1), f32)], axis=1
    )
    both = jnp.concatenate([tastes(1, 1 - n).astype(f32).reshape(QUAD * K, LANES), near], axis=0)
    ring = [(2 * i + j, (i + 1) % 4 * 2 + 1 - j) for i in range(4) for j in range(2)]
    both = lax.ppermute(both, ("draw", "nest"), ring)
    others = []
    for shift in (2, 3):
        others.append(lax.ppermute(tastes(shift, n), "draw", [(i, (i + shift) % 4) for i in range(4)]))
    rows = len(PLACES) * HALF
    plan = pl.pallas_call(
        arrange,
        name="arrange",
        out_shape=(
            jax.ShapeDtypeStruct((NESTS + K + NESTS, LANES), f32),
            jax.ShapeDtypeStruct((rows, DRAWS), bf16),
            jax.ShapeDtypeStruct((rows, LANES), bf16),
            jax.ShapeDtypeStruct((rows, LANES), bf16),
        ),
        in_specs=[VMEM] * 3,
        out_specs=(VMEM,) * 4,
        cost_estimate=pl.CostEstimate(flops=2_000_000, bytes_accessed=2_000_000, transcendentals=0),
        compiler_params=pltpu.CompilerParams(vmem_limit_bytes=4 * MIB),
    )(near, both, taste_scale.reshape(1, K))
    results = pl.pallas_call(
        contract,
        name="contract",
        out_shape=jax.ShapeDtypeStruct((8, 32, LANES), f32),
        in_specs=[VMEM] * 9,
        out_specs=VMEM,
        scratch_shapes=[
            pltpu.VMEM((rows, 2 * LANES), bf16),
            pltpu.VMEM((QUAD, 2 * LANES, DRAWS), bf16),
            pltpu.VMEM((BLOCKS * ROWS, LANES), f32),
        ],
        compiler_params=pltpu.CompilerParams(vmem_limit_bytes=36 * MIB),
    )(recv, tastes(0, n), both, *others, *plan)
    gathered = lax.all_to_all(results, ("draw", "nest"), split_axis=0, concat_axis=0, tiled=True)
    shape = jax.ShapeDtypeStruct((32, HALF * SLOTS), f32)
    return pl.pallas_call(
        unpack,
        name="unpack",
        out_shape=(shape, shape),
        in_specs=[VMEM],
        out_specs=(VMEM, VMEM),
        compiler_params=pltpu.CompilerParams(vmem_limit_bytes=2 * MIB),
    )(gathered.reshape(256, LANES))


def solution(mesh):
    in_specs = (
        P(None, "mkt", None),
        P("mkt", None, "draw"),
        P(),
        P("nest"),
        P("nest", None),
        P("mkt", None),
    )
    out_specs = (P("mkt", "nest"), P("mkt", "nest"))


    return jax.shard_map(shards, mesh=mesh, in_specs=in_specs, out_specs=out_specs, check_vma=False)
```

```python
import math

import jax
import jax.numpy as jnp
from jax import lax
from jax.experimental import pallas as pl
from jax.experimental.pallas import tpu as pltpu
from jax.sharding import PartitionSpec as P


ITERS = 3
BLOCKS = 32
QUAD = 4
K = 32
PROD = 16
SLOTS = 48
NESTS = 16
HALF = 8
WIDE = 24
DRAWS = 512
MARKETS = 1024
LANES = 128
ROWS = 18
LOG2E = 1.0 / math.log(2.0)
LOW = -1e30
MIB = 1024 * 1024
TINY = 1.1754944e-38
EMPTY = 32 * 16 + 15
CUT = 32
PLACES = [(o, t) for t in range(CUT) for o in range(2)] + [(o, t) for o in range(2) for t in range(CUT, SLOTS)]
SHORT = len(PLACES) - (SLOTS - CUT)
f32, bf16, i32 = jnp.float32, jnp.bfloat16, jnp.int32
VMEM = pl.BlockSpec(memory_space=pltpu.VMEM)
HBM = pl.BlockSpec(memory_space=pltpu.HBM)
PARTS = 2


def iota(shape, dim):
    return lax.broadcasted_iota(i32, shape, dim)


def dot(a, b):
    return lax.dot_general(a, b, (((1,), (0,)), ((), ())), preferred_element_type=f32)


def dot_t(a, b):
    return lax.dot_general(a, b, (((1,), (1,)), ((), ())), preferred_element_type=f32)


def pack(f_hbm, l_hbm, taste_hbm, members_hbm, rate_hbm, out_hbm, both_ref, t0_ref, t2_ref, t3_ref,
         f_ref, l_ref, taste_ref, members_ref, rate_ref, g_ref, o_ref, out_ref, sems):
    loads = [pltpu.make_async_copy(l_hbm, l_ref, sems.at[PARTS])]
    for c in range(PARTS):
        part = pl.ds(c * K // PARTS, K // PARTS)
        loads.append(pltpu.make_async_copy(f_hbm.at[part], f_ref.at[part], sems.at[c]))
    d, n = lax.axis_index("draw"), lax.axis_index("nest")
    first = lax.rem(d + 1, 4) * 8 + (1 - n) * QUAD
    loads.append(pltpu.make_async_copy(taste_hbm.at[pl.ds(first, QUAD)], taste_ref, sems.at[PARTS + 1]))
    loads.append(pltpu.make_async_copy(members_hbm, members_ref, sems.at[PARTS + 2]))
    loads.append(pltpu.make_async_copy(rate_hbm, rate_ref, sems.at[PARTS + 3]))
    for c, (shift, ref) in enumerate(((0, t0_ref), (2, t2_ref), (3, t3_ref))):
        start = lax.rem(d + shift, 4) * 8 + n * QUAD
        loads.append(pltpu.make_async_copy(taste_hbm.at[pl.ds(start, QUAD)], ref, sems.at[PARTS + 4 + c]))
    for load in loads:
        load.start()
    base = (d * 2 + n) * QUAD
    market = iota((MARKETS, LANES), 0)
    lane = iota((MARKETS, LANES), 1)
    pick = jnp.where(market == (lane % BLOCKS) * 32 + base + lane // BLOCKS, 1.0, 0.0).astype(bf16)
    spread = jnp.where(iota((BLOCKS, LANES), 0) == iota((BLOCKS, LANES), 1) % BLOCKS, 1.0, 0.0).astype(bf16)

    loads[0].wait()
    log = l_ref[...]
    high = log.astype(bf16)
    rest = log - high.astype(f32)
    middle = rest.astype(bf16)
    low = (rest - middle.astype(f32)).astype(bf16)
    logs = dot(jnp.concatenate([high, middle, low], axis=0), pick)
    own = (iota((LANES, LANES), 0) // PROD) % QUAD == iota((LANES, LANES), 1) // BLOCKS
    first = jnp.concatenate([logs[:PROD]] * QUAD + [logs[PROD : 2 * PROD]] * QUAD, axis=0)
    second = jnp.concatenate([logs[2 * PROD :]] * QUAD + [jnp.zeros((64, LANES), f32)], axis=0)
    o_ref[pl.ds(PROD, BLOCKS, stride=ROWS), :] = dot_t(spread, jnp.where(own, first, 0.0).astype(bf16))
    o_ref[pl.ds(PROD + 1, BLOCKS, stride=ROWS), :] = dot_t(spread, jnp.where(own, second, 0.0).astype(bf16))

    for load in loads[1 + PARTS : 4 + PARTS]:
        load.wait()
    both_ref[: QUAD * K, :] = taste_ref[...].astype(f32).reshape(QUAD * K, LANES)
    both_ref[QUAD * K :, :] = jnp.zeros((HALF, LANES), f32)
    both_ref[QUAD * K :, :SLOTS] = members_ref[...].astype(f32)
    square = iota((HALF, HALF), 0) == iota((HALF, HALF), 1)
    rates = jnp.where(square, jnp.broadcast_to(rate_ref[...], (HALF, HALF)), 0.0)
    rates = jnp.broadcast_to(jnp.sum(rates, axis=1, keepdims=True), (HALF, LANES))
    nests = jnp.where(iota((HALF, LANES), 1) == SLOTS, rates, both_ref[QUAD * K :, :])
    both_ref[QUAD * K :, :] = nests

    rows = K * PROD // PARTS
    for c in range(PARTS):
        loads[1 + c].wait()
        part = f_ref[c * K // PARTS : (c + 1) * K // PARTS].reshape(rows, MARKETS)
        g_ref[c * rows : (c + 1) * rows, :] = dot(part, pick)
    own = iota((LANES, LANES), 0) // K == iota((LANES, LANES), 1) // BLOCKS
    parts = []
    for j in range(PROD):
        part = g_ref[pl.ds(j, K, stride=PROD), :]
        parts.append(jnp.where(own, jnp.concatenate([part] * QUAD, axis=0), 0.0).astype(bf16))
    goods = dot_t(spread, jnp.concatenate(parts, axis=0))
    for j in range(PROD):
        o_ref[pl.ds(j, BLOCKS, stride=ROWS), :] = goods[:, j * LANES : (j + 1) * LANES]
    stores = []
    half = BLOCKS * ROWS // 2
    for c in range(2):
        out_ref[c * half : (c + 1) * half, :] = o_ref[c * half : (c + 1) * half, :].astype(bf16)
        part = pl.ds(c * half, half)
        stores.append(pltpu.make_async_copy(out_ref.at[part], out_hbm.at[part], sems.at[c]))
        stores[-1].start()
    for copy in loads[4 + PARTS :] + stores:
        copy.wait()


def across(x):
    return jnp.concatenate([x] * (DRAWS // LANES), axis=1)


def arrange(near_ref, next_ref, scale_ref, table_ref, hot_ref, pick_ref, mask_ref):
    first = lax.axis_index("nest") == 0
    near, far = near_ref[QUAD * K :, :], next_ref[QUAD * K :, :]
    table = jnp.concatenate([jnp.where(first, near, far), jnp.where(first, far, near)], axis=0)
    row, lane = iota((NESTS, LANES), 0), iota((NESTS, LANES), 1)
    filled = jnp.where((lane < SLOTS) & (table >= 0.0), 1.0, 0.0)
    size = jnp.broadcast_to(jnp.sum(filled, axis=1, keepdims=True), (NESTS, LANES))
    across_size = jnp.sum(jnp.where(row == lane, size, 0.0), axis=0, keepdims=True)
    ahead = (across_size > size) | ((across_size == size) & (lane < row))
    ahead = jnp.where(ahead & (lane < NESTS), 1.0, 0.0)
    rank = jnp.broadcast_to(jnp.sum(ahead, axis=1, keepdims=True), (NESTS, LANES))
    across_rank = jnp.sum(jnp.where(row == lane, rank, 0.0), axis=0, keepdims=True)
    place = jnp.where((across_rank == row.astype(f32)) & (lane < NESTS), 1.0, 0.0)
    ordered = table
    for g in range(NESTS):
        chosen = jnp.broadcast_to(place[:, g : g + 1], (NESTS, LANES)) > 0.5
        ordered = jnp.where(chosen, jnp.broadcast_to(table[g : g + 1, :], (NESTS, LANES)), ordered)
    table = ordered
    table_ref[:NESTS, :] = table
    table_ref[NESTS + K :, :] = rank
    square = iota((K, K), 0) == iota((K, K), 1)
    scale = jnp.sum(jnp.where(square, jnp.broadcast_to(scale_ref[...], (K, K)), 0.0), axis=1, keepdims=True)
    table_ref[NESTS : NESTS + K, :] = jnp.broadcast_to(scale, (K, LANES))
    ids = table.astype(i32)
    ids = jnp.where(ids < 0, EMPTY, ids)
    wide, narrow = iota((HALF, DRAWS), 1), iota((HALF, LANES), 1)
    for b in range(0, len(PLACES), 2):
        hot, pick, mask = [], [], []
        for o, t in PLACES[b : b + 2]:
            here = jnp.broadcast_to(ids[o * HALF : (o + 1) * HALF, t : t + 1], (HALF, LANES))
            hot.append(jnp.where(across(here) == wide, 1.0, 0.0))
            pick.append(jnp.where((here >> 4) == narrow, 1.0, 0.0))
            mask.append(jnp.where((here & 15) == (narrow & 15), 1.0, 0.0))
        rows = slice(b * HALF, (b + 2) * HALF)
        hot_ref[rows, :] = jnp.concatenate(hot, axis=0).astype(bf16)
        pick_ref[rows, :] = jnp.concatenate(pick, axis=0).astype(bf16)
        mask_ref[rows, :] = jnp.concatenate(mask, axis=0).astype(bf16)


def solve(count, x_ref, taste_refs, table_ref, hot_ref, pick_ref, mask_ref, out_ref, slot_ref, taste_ref, l_ref):
    used = count * HALF
    table = [table_ref[o * HALF : (o + 1) * HALF, :] for o in range(2)]
    rate = [jnp.broadcast_to(x[:, SLOTS : SLOTS + 1], (HALF, LANES)) for x in table]
    inverse = [1.0 / x for x in rate]
    to_two = [across(LOG2E * x) for x in inverse]
    gain = [(1.0 - x) * y[:, :LANES] for x, y in zip(rate, to_two)]
    less = [across((x - 1.0) * LOG2E) for x in rate]
    narrow = iota((HALF, LANES), 1)

    l_ref[...] = x_ref[...].astype(f32)
    top = l_ref[pl.ds(PROD, BLOCKS, stride=ROWS), :]
    rest = l_ref[pl.ds(PROD + 1, BLOCKS, stride=ROWS), :]
    both = jnp.concatenate([top, rest], axis=1)
    lane = iota((BLOCKS, 2 * LANES), 1)
    lows = (iota((BLOCKS, 2 * LANES), 0) == 0) & (lane < 64) & (lane % PROD == PROD - 1)
    both = jnp.concatenate([both, jnp.where(lows, LOW, 0.0), jnp.zeros((64, 2 * LANES), f32)], axis=0).astype(bf16)
    rows = dot(pick_ref[:used, :], both).astype(bf16)
    mask = mask_ref[:used, :]
    rows = rows * jnp.concatenate([mask, mask], axis=1)
    source, lane = iota((2 * LANES, 2 * LANES), 0), iota((2 * LANES, 2 * LANES), 1)
    market = (source // PROD) % QUAD
    fold = ((lane < LANES) & ((source // 64) * QUAD + market == lane)) | ((lane >= LANES) & (market == lane // 32 - QUAD))
    folded = dot(rows, jnp.where(fold, 1.0, 0.0).astype(bf16))
    goals = folded[:, LANES:]
    ones = jnp.where((narrow >= 3 * QUAD) & (narrow < 3 * QUAD + 3), 1.0, 0.0)
    slot_ref[:used, LANES:] = (folded[:, :LANES] + jnp.concatenate([ones] * count, axis=0)).astype(bf16)
    whole = (top + pltpu.roll(top, 64, 1)) + rest
    shares = jnp.exp(whole)
    column = iota((BLOCKS, LANES), 1)
    outside = []
    for q in range(QUAD):
        inside = jnp.where(column // PROD == q, shares, 0.0)
        total = 1.0 - jnp.sum(jnp.sum(inside, axis=1, keepdims=True), axis=0, keepdims=True)
        outside.append(jnp.log(jnp.broadcast_to(total, (NESTS, LANES))))

    x = jnp.concatenate([l_ref[i * ROWS : i * ROWS + PROD, :] for i in range(BLOCKS)], axis=0).astype(bf16)
    slot_ref[:used, :LANES] = dot(hot_ref[:used, :], x).astype(bf16)
    scale = table_ref[NESTS : NESTS + K, :]
    taste_ref[...] = jnp.zeros_like(taste_ref)
    for q in range(QUAD):
        for b, ref in enumerate(taste_refs):
            taste = ref[q] if b != 1 else ref[q * K : (q + 1) * K, :]
            taste = (scale * taste.astype(f32)).astype(bf16)
            taste_ref[q, q * K : (q + 1) * K, b * LANES : (b + 1) * LANES] = taste
        row = iota((NESTS, LANES), 0)
        start = jnp.where((row < 3 * QUAD) & (row % QUAD == q), 1.0, 0.0)
        rest = -outside[q]
        for part in range(3):
            piece = rest.astype(bf16).astype(f32)
            start = jnp.where(row == 3 * QUAD + part, piece, start)
            rest = rest - piece
        taste_ref[q, LANES : LANES + NESTS, :] = across(start).astype(bf16)

    def weights(inner):
        power = [jnp.exp2(x * jnp.log(y)) for x, y in zip(less, inner)]
        total = jnp.sum(power[0] * inner[0] + power[1] * inner[1], axis=0, keepdims=True)
        total = (1.0 + total) * DRAWS
        return [x / total for x in power]

    def exps(q, b, inner, power):
        o = PLACES[b][0]
        e = jnp.exp2(power)
        held[q, b] = e
        inner[o] = inner[o] + e

    def collect(b, tiles, copies):
        o, t = PLACES[b]
        tiles[o] = jnp.where(narrow == t, copies, tiles[o])

    def sums(q, b, weight, share):
        p = held[q, b] * weight[PLACES[b][0]]
        p = (p[:, :128] + p[:, 128:256]) + (p[:, 256:384] + p[:, 384:])
        collect(b, share, jnp.broadcast_to(jnp.sum(p, axis=1, keepdims=True), (HALF, LANES)))

    zeros = jnp.zeros((HALF, DRAWS), f32)
    held, base = {}, {}
    blank = jnp.zeros((HALF, LANES), f32)
    weight, target, value, share = [[None] * QUAD for _ in range(4)]
    for q in range(QUAD):
        mu = dot(slot_ref[:used, :], taste_ref[q])
        inner = [zeros, zeros]
        for b, (o, _) in enumerate(PLACES[:count]):
            part = mu[b * HALF : (b + 1) * HALF] * to_two[o]
            base[q, b] = part
            exps(q, b, inner, part)
        weight[q] = weights(inner)
        value[q] = [blank, blank]

    tiles = [[blank, blank], [blank, blank]]
    for b, (o, t) in enumerate(PLACES[:count]):
        tile = tiles[t // 32]
        tile[o] = jnp.where(narrow % 32 == t % 32, goals[b * HALF : (b + 1) * HALF], tile[o])
    for q in range(QUAD):
        target[q] = [
            jnp.where(narrow < 32, pltpu.roll(x, (128 - 32 * q) % 128, 1), pltpu.roll(y, (160 - 32 * q) % 128, 1))
            for x, y in zip(*tiles)
        ]

    lag = 1
    for stage in range(ITERS * QUAD):
        q = stage % QUAD
        ahead = stage - lag if 0 <= stage - lag < (ITERS - 1) * QUAD else None
        share[q], inner = [blank, blank], [zeros, zeros]
        for b in range(count):
            sums(q, b, weight[q], share[q])
            if ahead is not None:
                o, t = PLACES[b]
                move = jnp.broadcast_to(value[ahead % QUAD][o][:, t : t + 1], (HALF, LANES))
                exps(ahead % QUAD, b, inner, base[ahead % QUAD, b] + across(move))
        if ahead is not None:
            weight[ahead % QUAD] = weights(inner)
        value[q] = [
            v + g * (x - jnp.log(jnp.maximum(y, TINY))) for v, g, x, y in zip(value[q], gain, target[q], share[q])
        ]

    ranks = table_ref[NESTS + K :, :]
    whole_lane = iota((NESTS, LANES), 1)
    finals = []
    for q in range(QUAD):
        final = jnp.zeros((NESTS, LANES), f32)
        for o in range(2):
            result = (target[q][o] - outside[q][:HALF]) + value[q][o] * (rate[o] * math.log(2.0))
            result = jnp.where(table[o] >= 0.0, result, 0.0)
            result = jnp.where(narrow < SLOTS, result, pltpu.roll(share[q][o], SLOTS, 1))
            for r in range(HALF):
                one = jnp.broadcast_to(result[r : r + 1, :], (NESTS, LANES))
                final = jnp.where(ranks == float(o * HALF + r), one, final)
        finals.append(final)
    for q in range(QUAD - 1):
        last = pltpu.roll(finals[QUAD - 1], 96 - 32 * q, 1)
        final = jnp.where(whole_lane < 2 * SLOTS, finals[q], last)
        for n in range(2):
            for d in range(4):
                out_ref[2 * d + n, q * HALF : (q + 1) * HALF, :] = final[n * HALF : (n + 1) * HALF]


def contract(x_ref, t0_ref, t1_ref, t2_ref, t3_ref, table_ref, hot_ref, pick_ref, mask_ref, out_ref,
             slot_ref, taste_ref, l_ref):
    inputs = (x_ref, (t0_ref, t1_ref, t2_ref, t3_ref), table_ref, hot_ref, pick_ref, mask_ref, out_ref)
    short = table_ref[HALF, CUT] < 0.0

    @pl.when(short)
    def _():
        solve(SHORT, *inputs, slot_ref, taste_ref, l_ref)

    @pl.when(jnp.logical_not(short))
    def _():
        solve(len(PLACES), *inputs, slot_ref, taste_ref, l_ref)


def unpack(r_ref, value_ref, share_ref, rows_ref):
    lane = iota((8, LANES), 1)
    for g in range(HALF):
        parts = [r_ref[pl.ds(q * HALF + g, 8, stride=WIDE), :] for q in range(QUAD - 1)]
        last = [pltpu.roll(x, 32 * (q + 1), 1) for q, x in enumerate(parts)]
        parts.append(jnp.where(lane < 32, last[0], jnp.where(lane < 64, last[1], last[2])))
        for q, part in enumerate(parts):
            rows_ref[pl.ds(g * 32 + q, 8, stride=QUAD), :] = part
        part = rows_ref[g * 32 : (g + 1) * 32, :]
        value_ref[:, g * SLOTS : (g + 1) * SLOTS] = part[:, :SLOTS]
        share_ref[:, g * SLOTS : (g + 1) * SLOTS] = part[:, SLOTS : 2 * SLOTS]


def shards(features, taste_draws, taste_scale, nest_param, members, log_share):
    inputs = (features, log_share, taste_draws, members, nest_param.reshape(1, HALF))
    tastes = jax.ShapeDtypeStruct((QUAD, K, LANES), bf16)
    send, near, *tastes = pl.pallas_call(
        pack,
        name="pack",
        out_shape=(
            jax.ShapeDtypeStruct((BLOCKS * ROWS, LANES), bf16),
            jax.ShapeDtypeStruct((QUAD * K + HALF, LANES), f32),
            *[tastes] * 3,
        ),
        in_specs=[HBM] * 5,
        out_specs=(HBM, VMEM, VMEM, VMEM, VMEM),
        scratch_shapes=[
            pltpu.VMEM((K, PROD, MARKETS), bf16),
            pltpu.VMEM((PROD, MARKETS), f32),
            pltpu.VMEM((QUAD, K, LANES), bf16),
            pltpu.VMEM((HALF, SLOTS), i32),
            pltpu.VMEM((1, HALF), f32),
            pltpu.VMEM((K * PROD, LANES), f32),
            pltpu.VMEM((BLOCKS * ROWS, LANES), f32),
            pltpu.VMEM((BLOCKS * ROWS, LANES), bf16),
            pltpu.SemaphoreType.DMA((PARTS + 7,)),
        ],
        compiler_params=pltpu.CompilerParams(vmem_limit_bytes=8 * MIB),
    )(*(pltpu.with_memory_space_constraint(x, pltpu.HBM) for x in inputs))
    send = send.reshape(BLOCKS, ROWS // 2, 2, LANES)
    recv = lax.all_to_all(send, "mkt", split_axis=0, concat_axis=0, tiled=True)
    recv = recv.reshape(BLOCKS * ROWS, LANES)

    ring = [(2 * i + j, (i + 1) % 4 * 2 + 1 - j) for i in range(4) for j in range(2)]
    both = lax.ppermute(near, ("draw", "nest"), ring)
    for shift in (2, 3):
        ring = [(i, (i + shift) % 4) for i in range(4)]
        tastes[shift - 1] = lax.ppermute(tastes[shift - 1], "draw", ring)
    rows = len(PLACES) * HALF
    plan = pl.pallas_call(
        arrange,
        name="arrange",
        out_shape=(
            jax.ShapeDtypeStruct((NESTS + K + NESTS, LANES), f32),
            jax.ShapeDtypeStruct((rows, DRAWS), bf16),
            jax.ShapeDtypeStruct((rows, LANES), bf16),
            jax.ShapeDtypeStruct((rows, LANES), bf16),
        ),
        in_specs=[VMEM] * 3,
        out_specs=(VMEM,) * 4,
        cost_estimate=pl.CostEstimate(flops=2_000_000, bytes_accessed=2_000_000, transcendentals=0),
        compiler_params=pltpu.CompilerParams(vmem_limit_bytes=4 * MIB),
    )(near, both, taste_scale.reshape(1, K))
    results = pl.pallas_call(
        contract,
        name="contract",
        out_shape=jax.ShapeDtypeStruct((8, WIDE, LANES), f32),
        in_specs=[VMEM] * 9,
        out_specs=VMEM,
        scratch_shapes=[
            pltpu.VMEM((rows, 2 * LANES), bf16),
            pltpu.VMEM((QUAD, 2 * LANES, DRAWS), bf16),
            pltpu.VMEM((BLOCKS * ROWS, LANES), f32),
        ],
        compiler_params=pltpu.CompilerParams(vmem_limit_bytes=36 * MIB),
    )(recv, tastes[0], both, *tastes[1:], *plan)
    gathered = lax.all_to_all(results, ("draw", "nest"), split_axis=0, concat_axis=0, tiled=True)
    shape = jax.ShapeDtypeStruct((32, HALF * SLOTS), f32)
    return pl.pallas_call(
        unpack,
        name="unpack",
        out_shape=(shape, shape),
        in_specs=[VMEM],
        out_specs=(VMEM, VMEM),
        scratch_shapes=[pltpu.VMEM((8 * 32, LANES), f32)],
        compiler_params=pltpu.CompilerParams(vmem_limit_bytes=2 * MIB),
    )(gathered.reshape(8 * WIDE, LANES))


def solution(mesh):
    in_specs = (
        P(None, "mkt", None),
        P("mkt", None, "draw"),
        P(),
        P("nest"),
        P("nest", None),
        P("mkt", None),
    )
    out_specs = (P("mkt", "nest"), P("mkt", "nest"))


    return jax.shard_map(shards, mesh=mesh, in_specs=in_specs, out_specs=out_specs, check_vma=False)
```
